32 devices in a mesh: lon: 2 (over x), lat: 4 (over y, core), head: 4 (over z).
Axes of the slice: x: 2, y: 2, z: 4, core: 2. Of those that a mesh axis runs over, the one named last changes fastest.
Arguments:
- features: bfloat16 [8, 24, 24, 384], P(None, 'lat', 'lon'), may hold values from -6 to 6
- attend_weight: bfloat16 [3, 384, 384], P(None, None, 'head'), may hold values from -0.3125 to 0.3125
- output_weight: bfloat16 [384, 384], P('head'), may hold values from -0.3125 to 0.3125
- bias_table: float32 [64, 12, 3312], P(None, 'head'), may hold values from -3 to 304
- bias_type: int32 [4, 4], P(None, 'lat'), may hold values from 0 to 63
- window_shift: int32 [1], replicated, may hold values from 1 to 11
- grad_out: bfloat16 [8, 24, 24, 384], P(None, 'lat', 'lon'), may hold values from -6 to 6
Outputs:
- feature_grad: bfloat16 [8, 24, 24, 384], P(None, 'lat', 'lon', 'head')
- attend_grad: float32 [3, 384, 384], P(None, None, 'head')
- output_grad: float32 [384, 384], P('head')
- bias_grad: float32 [64, 12, 3312], P(None, 'head')
The draws below stay inside these ranges and needn't reach their ends.
All inputs are finite; a program needn't handle non-finite values.
Results may differ from the reference program's by a relative error of at most 0.01.
Values may be sent and summed in bfloat16 or wider, within the bound.
A program may use at most 128 MiB of HBM per device.

```python
import jax
import jax.numpy as jnp
import numpy as np
from jax import lax

D = 384
HEADS = 12
TYPES = 64
WIN_LEVEL = 2
WIN_LAT = 6
WIN_LON = 12
REL_COUNT = 3312
LEVELS = 8
LAT = 24
LON = 24
LEVEL_WINS = 4
LAT_WINS = 4
N_HEAD = 4


def draw_bias_table(key, part):
    base_key = jax.random.fold_in(key, 11)
    first_key = jax.random.fold_in(base_key, 0)
    table = jnp.clip(jax.random.normal(first_key, (TYPES, HEADS, REL_COUNT), jnp.float32), -3.0, 3.0)
    return table


def with_ends(values, key, smallest, top_value):
    spot = [jax.random.randint(jax.random.fold_in(key, axis), (), 0, length) for axis, length in enumerate(values.shape)]
    main_axis = values.shape.index(max(values.shape))
    next_to = spot[:main_axis] + [(spot[main_axis] + 1) % values.shape[main_axis]] + spot[main_axis + 1:]
    return values.at[tuple(spot)].set(smallest).at[tuple(next_to)].set(top_value)


def levels(rng, extent, shards, least, high):
    gain, own = 1.0, jax.random.fold_in(rng, 6)
    for dim, shards_of in shards:
        heights = jnp.exp(jax.random.uniform(jax.random.fold_in(own, dim), (shards_of,), jnp.float32, least / len(shards), high / len(shards)))
        gain = gain * jnp.repeat(heights, extent[dim] // shards_of).reshape([-1 if axis == dim else 1 for axis in range(len(extent))])
    return gain


def centred(own_key, dims, width, most, cuts=(), held_as=jnp.bfloat16):
    gain = levels(own_key, dims, cuts, -0.22, 0.18) if cuts else 1.0
    entries = jax.random.normal(own_key, dims, jnp.float32) * width * gain
    return jnp.minimum(jnp.maximum(entries, -most), most).astype(held_as)


def setup_inputs(seed: int = 0) -> dict:
    seeds = jax.random.split(jax.random.key(seed), 8)
    return {
        "features": centred(seeds[0], (LEVELS, LAT, LON, D), 1.0, 6.0, ((1, 4), (2, 2))),
        "attend_weight": centred(seeds[1], (3, D, D), D ** -0.5, 0.3125, ((2, 4),)),
        "output_weight": centred(seeds[2], (D, D), D ** -0.5, 0.3125, ((0, 4),)),
        "bias_table": draw_bias_table(jax.random.fold_in(seeds[7], 71), 0),
        "bias_type": with_ends(jax.random.randint(seeds[4], (LEVEL_WINS, LAT_WINS), 0, TYPES), jax.random.fold_in(seeds[4], 1), 0, TYPES - 1).astype(jnp.int32),
        "window_shift": jax.random.randint(seeds[5], (1,), 1, WIN_LON).astype(jnp.int32),
        "grad_out": centred(seeds[6], (LEVELS, LAT, LON, D), 1.0, 6.0, ((1, 4), (2, 2))),
    }


def relative_index(win_level, win_lat, win_lon):
    level_pos, lat_pos, lon_pos = np.meshgrid(np.arange(win_level), np.arange(win_lat), np.arange(win_lon), indexing="ij")
    level_pos = level_pos.reshape(-1)
    lat_pos = lat_pos.reshape(-1)
    lon_pos = lon_pos.reshape(-1)
    pair_level = level_pos[:, None] * win_level + level_pos[None, :]
    pair_lat = lat_pos[:, None] * win_lat + lat_pos[None, :]
    offset_lon = lon_pos[:, None] - lon_pos[None, :] + win_lon - 1
    combined = (pair_level * win_lat * win_lat + pair_lat) * (2 * win_lon - 1) + offset_lon
    return jnp.asarray(combined.reshape(-1).astype(np.int32))


def halve(values):
    return lax.optimization_barrier(values.astype(jnp.bfloat16)).astype(jnp.float32)


def attend_backward(tokens, grad_rows, window_types, attend_weight, output_weight, bias_table, relation):
    outer_count, inner_count, win_tokens, model_width = tokens.shape
    head_count = bias_table.shape[1]
    head_size = attend_weight.shape[2] // head_count
    scaling = head_size ** -0.5
    tokens_full = tokens.astype(jnp.float32)
    grad_full = grad_rows.astype(jnp.float32)
    projected = halve(jnp.einsum("abnd,cdk->cabnk", tokens_full, attend_weight.astype(jnp.float32)))
    split = projected.reshape(3, outer_count, inner_count, win_tokens, head_count, head_size)
    queries, key_rows, values = split[0], split[1], split[2]
    table_rows = jnp.take(bias_table, window_types, axis=0)
    bias_full = jnp.take(table_rows, relation, axis=2).reshape(outer_count, head_count, win_tokens, win_tokens)
    scores = jnp.einsum("abihe,abjhe->abhij", queries, key_rows) * scaling + bias_full[:, None]
    softened = jax.nn.softmax(scores, axis=-1)
    softened_half = halve(softened)
    attended = halve(jnp.einsum("abhij,abjhe->abihe", softened_half, values))
    grad_attended = halve(jnp.einsum("abnd,kd->abnk", grad_full, output_weight.astype(jnp.float32)))
    grad_heads = grad_attended.reshape(outer_count, inner_count, win_tokens, head_count, head_size)
    grad_values = halve(jnp.einsum("abhij,abihe->abjhe", softened_half, grad_heads))
    grad_softened = jnp.einsum("abihe,abjhe->abhij", grad_heads, values)
    grad_scores = softened * (grad_softened - jnp.sum(softened * grad_softened, axis=-1, keepdims=True))
    grad_scores_half = halve(grad_scores)
    grad_queries = halve(jnp.einsum("abhij,abjhe->abihe", grad_scores_half, key_rows) * scaling)
    grad_keys = halve(jnp.einsum("abhij,abihe->abjhe", grad_scores_half, queries) * scaling)
    grad_projected = jnp.stack([grad_queries, grad_keys, grad_values]).reshape(3, outer_count, inner_count, win_tokens, head_count * head_size)
    attended = attended.reshape(outer_count, inner_count, win_tokens, head_count * head_size)
    return attended, grad_projected, grad_scores


def reference(features, attend_weight, output_weight, bias_table, bias_type, window_shift, grad_out):
    offset = window_shift[0]
    rolled = jnp.roll(features, -offset, axis=2)
    rolled_grad = jnp.roll(grad_out, -offset, axis=2)
    relation = relative_index(WIN_LEVEL, WIN_LAT, WIN_LON)
    lon_wins = LON // WIN_LON
    level_wins = LEVELS // WIN_LEVEL
    win_tokens = WIN_LEVEL * WIN_LAT * WIN_LON
    head_count = bias_table.shape[1]
    rel_total = bias_table.shape[2]
    group_cols = D // N_HEAD

    def to_windows(band):
        shaped = band.reshape(level_wins, WIN_LEVEL, WIN_LAT, lon_wins, WIN_LON, D)
        return shaped.transpose(0, 3, 1, 2, 4, 5).reshape(level_wins, lon_wins, win_tokens, D)

    def from_windows(windows):
        shaped = windows.reshape(level_wins, lon_wins, WIN_LEVEL, WIN_LAT, WIN_LON, D)
        return shaped.transpose(0, 2, 3, 1, 4, 5).reshape(LEVELS, WIN_LAT, LON, D)

    def band_step(totals, band_index):
        grad_attend, grad_output, grad_bias = totals
        band_start = band_index * WIN_LAT
        tokens = to_windows(lax.dynamic_slice_in_dim(rolled, band_start, WIN_LAT, 1))
        grad_rows = to_windows(lax.dynamic_slice_in_dim(rolled_grad, band_start, WIN_LAT, 1))
        window_types = lax.dynamic_slice_in_dim(bias_type, band_index, 1, 1)[:, 0].astype(jnp.int32)
        attended, grad_projected, grad_scores = attend_backward(tokens, grad_rows, window_types, attend_weight, output_weight, bias_table, relation)
        tokens_full = tokens.astype(jnp.float32)
        grad_attend = grad_attend + jnp.einsum("abnd,cabnk->cdk", tokens_full, grad_projected)
        grad_output = grad_output + jnp.einsum("abnk,abnd->kd", attended, grad_rows.astype(jnp.float32))
        summed_scores = jnp.sum(grad_scores, axis=1).reshape(-1)
        segment_ids = (window_types[:, None, None] * head_count * rel_total + jnp.arange(head_count, dtype=jnp.int32)[None, :, None] * rel_total + relation[None, None, :]).reshape(-1)
        grad_bias = grad_bias + jax.ops.segment_sum(summed_scores, segment_ids, num_segments=bias_table.shape[0] * head_count * rel_total).reshape(bias_table.shape)
        grouped = grad_projected.reshape(3, level_wins, lon_wins, win_tokens, N_HEAD, group_cols)
        weight_grouped = attend_weight.astype(jnp.float32).reshape(3, D, N_HEAD, group_cols)
        pieces = halve(jnp.einsum("cabngk,cdgk->gabnd", grouped, weight_grouped))
        band_grad = from_windows(jnp.sum(pieces, axis=0)).astype(jnp.bfloat16)
        return (grad_attend, grad_output, grad_bias), band_grad

    start_totals = (jnp.zeros((3, D, D), jnp.float32), jnp.zeros((D, D), jnp.float32), jnp.zeros(bias_table.shape, jnp.float32))
    totals, bands = lax.scan(band_step, start_totals, jnp.arange(LAT // WIN_LAT, dtype=jnp.int32))
    grid_grad = bands.transpose(1, 0, 2, 3, 4).reshape(LEVELS, LAT, LON, D)
    feature_grad = jnp.roll(grid_grad, offset, axis=2)
    return feature_grad, totals[0], totals[1], totals[2]
```

```python
import functools

import jax
import jax.numpy as jnp
from jax import lax
from jax.experimental import pallas as pl
from jax.experimental.pallas import tpu as pltpu
from jax.sharding import PartitionSpec as P

WIN_LEVEL = 2
WIN_LAT = 6
WIN_LON = 12
HALF = WIN_LON // 2
SPAN = 2 * WIN_LON - 1
SIDE = WIN_LON * WIN_LAT
TOK = WIN_LEVEL * SIDE
EDGE = HALF * WIN_LAT
MAIN = TOK - EDGE
PART = WIN_LAT * SPAN
LOG2E = 1.4426950408889634
F32 = jnp.float32
BF16 = jnp.bfloat16

NN = ((1,), (0,))
NT = ((1,), (1,))
TN = ((0,), (0,))


def dot(a, b, dims):
    return lax.dot_general(a, b, (dims, ((), ())), preferred_element_type=F32)


def up(n, to):
    return -(-n // to) * to


def bits_of(n):
    return [1 << k for k in range(n.bit_length() - 1)]


def flip(i, bit):
    return i + bit - 2 * bit * lax.rem(i // bit, 2)


def permutation():
    row = lax.broadcasted_iota(jnp.int32, (PART, 256), 0)
    out = lax.broadcasted_iota(jnp.int32, (PART, 256), 1)
    a, d = row // SPAN, row % SPAN
    place = jnp.where(d < WIN_LON, d * WIN_LAT + a, 128 + (d - WIN_LON) * WIN_LAT + a)
    return jnp.where(place == out, 1.0, 0.0).astype(BF16)


def lane_lon(lanes):
    return lax.broadcasted_iota(jnp.int32, (1, lanes), 1) % SIDE // WIN_LAT


def block_kernel(heads, shift_ref, type_ref, x_hbm, g_hbm, aw_hbm, ow_hbm, table_hbm,
                 own_ref, edge_ref, all_w_ref, all_bias_ref,
                 x_own, g_own, aw, ow, table, halo_f, own_f, halo_out, halo_in, xs, gs,
                 line, parts, bias, gbias, gp, aw_split, piece_out, piece_in, edge_out,
                 w_core, w_core_in, w_cur, w_in, bias_cur, bias_in,
                 local, halo_sem, piece_sem, edge_sem, w_sem, bias_sem):
    lons, lats, groups = (lax.axis_size(name) for name in ("lon", "lat", "head"))
    lon, lat, head = (lax.axis_index(name) for name in ("lon", "lat", "head"))
    shift = shift_ref[0]
    early = shift <= HALF
    cols, levels, width = x_own.shape[1:]
    wins = levels // WIN_LEVEL
    inner = aw.shape[1]
    size = inner // heads
    total = heads * TOK
    lanes = up(total, 128)
    tiles = lanes // 128

    loads = [
        pltpu.make_async_copy(src, dst, local.at[i])
        for i, (src, dst) in enumerate(
            ((x_hbm, x_own), (g_hbm, g_own), (table_hbm, table), (aw_hbm, aw), (ow_hbm, ow))
        )
    ]
    for load in loads:
        load.start()

    east = (lax.rem(lon + 1, lons), lat, head)
    west = (lax.rem(lon + lons - 1, lons), lat, head)
    lon_bits, lat_bits = bits_of(lons), bits_of(lats)
    mates = [(flip(lon, b), lat, head) for b in lon_bits]
    rows_up = [(lon, flip(lat, b), head) for b in lat_bits]
    sides = [east] if lons <= 2 else [east, west]
    peers = [(lon, lat, lax.rem(head + n, groups)) for n in range(1, groups)]
    greet = sides + (mates if lons > 2 else []) + rows_up + peers
    barrier = pltpu.get_barrier_semaphore()
    for device in greet:
        pl.semaphore_signal(barrier, inc=1, device_id=device, device_id_type=pl.DeviceIdType.MESH)

    def remote(src, dst, sems, k, device):
        return pltpu.make_async_remote_copy(
            src_ref=src, dst_ref=dst, send_sem=sems.at[0, k], recv_sem=sems.at[1, k],
            device_id=device, device_id_type=pl.DeviceIdType.MESH,
        )

    strips = width // 128

    def put(dst, i, spot, value):
        value = value.astype(F32)
        for t in range(strips):
            dst[i, t, spot * levels:(spot + 1) * levels, :] = value[:, t * 128:(t + 1) * 128]

    def take(src, i, level, count):
        rows = pl.ds(level, count, stride=levels)
        return jnp.concatenate([src[i, t, rows, :] for t in range(strips)], axis=1)

    loads[0].wait()
    loads[1].wait()
    sent = []
    for n in range(len(sides)):
        for i, src in enumerate((x_own, g_own)):
            for b in range(HALF):
                low = jnp.maximum(shift + b - HALF, 0)
                high = jnp.minimum(shift + b, cols - 1)
                if lons <= 2:
                    col = jnp.where(early, low, high)
                else:
                    col = high if n == 0 else low
                for a in range(WIN_LAT):
                    put(halo_f, i, b * WIN_LAT + a, src[a, col])
        for w in range(wins):
            for i in range(2):
                rows = [take(halo_f, i, WIN_LEVEL * w + z, EDGE) for z in range(WIN_LEVEL)]
                halo_out[n, w, i * 2 * EDGE:(i + 1) * 2 * EDGE, :] = jnp.concatenate(rows, axis=0).astype(BF16)
    pl.semaphore_wait(barrier, len(greet))
    for w in range(wins):
        for n, device in enumerate(sides):
            copy = remote(halo_out.at[n, w], halo_in.at[n, w], halo_sem, w * len(sides) + n, device)
            copy.start()
            sent.append(copy)

    for i, src in enumerate((x_own, g_own)):
        for b in range(WIN_LON):
            col = jnp.where(early, jnp.minimum(shift + b, cols - 1), jnp.maximum(shift + b - WIN_LON, 0))
            for a in range(WIN_LAT):
                put(own_f, i, b * WIN_LAT + a, src[a, col])

    loads[2].wait()
    parts[...] = jnp.zeros_like(parts)
    for h in range(heads):
        for w in range(wins):
            line[h * wins + w:h * wins + w + 1, :table.shape[2]] = table[h, pl.ds(type_ref[0, w], 1), :]
    block = WIN_LEVEL * WIN_LAT * wins
    spots = []
    for k in range(WIN_LEVEL * WIN_LEVEL * WIN_LAT * WIN_LAT):
        zi, zj = k // (WIN_LEVEL * WIN_LAT * WIN_LAT), k // (WIN_LAT * WIN_LAT) % WIN_LEVEL
        ai, aj = k // WIN_LAT % WIN_LAT, k % WIN_LAT
        for h in range(heads):
            seg = h * WIN_LEVEL + zi
            spots.append((k, h, seg * block + (zj * WIN_LAT + aj) * wins, ai * SPAN))
    for k, h, r, c in spots:
        parts[r:r + wins, c:c + SPAN] = line[h * wins:(h + 1) * wins, k * SPAN:(k + 1) * SPAN]
    perm = permutation()
    flat = parts[:, :PART]
    one = flat.astype(BF16)
    rest = flat - one.astype(F32)
    two = rest.astype(BF16)
    three = (rest - two.astype(F32)).astype(BF16)
    spread = (dot(one, perm, NN) + dot(two, perm, NN) + dot(three, perm, NN)) * LOG2E
    segs = heads * WIN_LEVEL
    pad = jnp.zeros((block, lanes - total), F32)

    def gathered(start):
        pieces = [spread[s * block:(s + 1) * block, start:start + SIDE] for s in range(segs)]
        return jnp.concatenate(pieces + [pad], axis=1)

    lower, upper = gathered(0), gathered(128)
    place = lane_lon(lanes)
    half = WIN_LAT * wins
    for b in range(WIN_LON):
        left = (lanes - WIN_LAT * (WIN_LON - 1 - b)) % lanes
        both = jnp.where(
            place <= b, pltpu.roll(lower, left, 1), pltpu.roll(upper, WIN_LAT * (b + 1), 1)
        )
        for z in range(WIN_LEVEL):
            r = (z * WIN_LON + b) * half
            for t in range(tiles):
                bias[t, r:r + half, :] = both[z * half:(z + 1) * half, t * 128:(t + 1) * 128]

    loads[3].wait()
    loads[4].wait()
    for c in range(3):
        for g in range(groups):
            chunk = aw[c, :, g * inner:(g + 1) * inner]
            aw_split[c, :, g * 128:(g + 1) * 128] = jnp.concatenate(
                [chunk, jnp.zeros((inner, 128 - inner), BF16)], axis=1
            )

    key_lon = lax.broadcasted_iota(jnp.int32, (TOK, 1), 0) % SIDE // WIN_LAT
    mine = jnp.where(early, (key_lon + shift < WIN_LON).astype(F32), (key_lon + shift >= WIN_LON).astype(F32)) > 0.5
    diag = (
        lax.broadcasted_iota(jnp.int32, (inner, lanes), 0) // size
        == lax.broadcasted_iota(jnp.int32, (inner, lanes), 1) // TOK
    )
    col_head = lax.broadcasted_iota(jnp.int32, (TOK, inner), 1) // size
    scaling = size ** -0.5

    def expanded(rows):
        rows = rows.astype(BF16).astype(F32)
        filled = jnp.concatenate([rows] * heads + [jnp.zeros((inner, lanes - total), F32)], axis=1)
        return jnp.where(diag, filled, 0.0).astype(BF16)

    def folded(wide_rows):
        out = jnp.zeros((TOK, inner), F32)
        for h in range(heads):
            out = jnp.where(col_head == h, wide_rows[h * TOK:(h + 1) * TOK], out)
        return out

    piece_copies = []

    def window(w):
        span = slice(w * TOK, (w + 1) * TOK)
        for n in range(len(sides)):
            sent[w * len(sides) + n].wait_recv()
        for i, dst in enumerate((xs, gs)):
            kept = [take(own_f, i, WIN_LEVEL * w + z, SIDE) for z in range(WIN_LEVEL)]
            kept = jnp.concatenate(kept, axis=0)
            near = [halo_in[n, w, i * 2 * EDGE:(i + 1) * 2 * EDGE, :].astype(F32) for n in range(len(sides))]
            first, last = (near[0], near[0]) if lons <= 2 else (near[0], near[1])
            filled = jnp.concatenate([first[:EDGE], last[:EDGE], first[EDGE:], last[EDGE:]], axis=0)
            dst[span, :] = jnp.where(mine, kept, filled).astype(BF16)
        tokens, grads = xs[span, :], gs[span, :]
        queries = expanded(dot(aw[0], tokens, NT))
        keys = dot(tokens, aw[1], NT).astype(BF16)
        values = dot(tokens, aw[2], NT).astype(BF16)
        gates = expanded(dot(ow[...], grads, NT))
        rows = pl.ds(w, TOK, stride=wins)
        offset = jnp.concatenate([bias[t, rows, :] for t in range(tiles)], axis=1)
        scores = dot(keys, queries, NN) * (scaling * LOG2E) + offset
        top = jnp.max(scores, axis=0, keepdims=True)
        raised = jnp.exp2(scores - top)
        soft = raised * (1.0 / jnp.sum(raised, axis=0, keepdims=True))
        soft_half = soft.astype(BF16)
        both = soft * dot(values, gates, NN)
        slopes = both - soft * jnp.sum(both, axis=0, keepdims=True)
        for t in range(tiles):
            gbias[t, rows, :] = slopes[:, t * 128:(t + 1) * 128]
        slopes_half = slopes.astype(BF16)
        gp[0, span, :] = (folded(dot(slopes_half, keys, TN)) * scaling).astype(BF16)
        gp[1, span, :] = (dot(slopes_half, queries, NT) * scaling).astype(BF16)
        gp[2, span, :] = dot(soft_half, gates, NT).astype(BF16)
        gp[3, span, :] = folded(dot(soft_half, values, TN)).astype(BF16)

    def send_pieces(w):
        span = slice(w * TOK, (w + 1) * TOK)
        out = sum(dot(gp[c, span, :], aw_split[c], NN) for c in range(3))
        for g in range(groups):
            chunk = out[:, g * 128:g * 128 + inner]
            tail = chunk[MAIN:]
            third = 128 - inner
            extra = jnp.concatenate([tail[:, t * third:(t + 1) * third] for t in range(inner // third)], axis=0)
            packed = jnp.concatenate([chunk[:MAIN], extra], axis=1).astype(BF16)
            piece_out[w, g, :MAIN, :] = packed
        for n, device in enumerate(peers):
            copy = remote(
                piece_out.at[w, device[2]], piece_in.at[w, n], piece_sem, w * len(peers) + n, device
            )
            copy.start()
            piece_copies.append(copy)

    edge_copies = []

    def sum_pieces(w):
        for n in range(len(peers)):
            piece_copies[w * len(peers) + n].wait_recv()
        got = piece_out[w, head].astype(F32)
        for n in range(len(peers)):
            got = got + piece_in[w, n].astype(F32)
        third = 128 - inner
        tail = [got[t * EDGE:(t + 1) * EDGE, inner:] for t in range(inner // third)]
        full = jnp.concatenate([got[:MAIN, :inner], jnp.concatenate(tail, axis=1)], axis=0)
        own_ref[w] = full.astype(BF16)
        first = jnp.concatenate([full[:EDGE], full[SIDE:SIDE + EDGE]], axis=0)
        last = jnp.concatenate([full[EDGE:SIDE], full[SIDE + EDGE:]], axis=0)
        if lons <= 2:
            outs = [jnp.where(early, last, first)]
        else:
            outs = [last, first]
        for n, device in enumerate(sides):
            edge_out[n, w] = outs[n].astype(BF16)
            copy = remote(edge_out.at[n, w], edge_ref.at[n, w], edge_sem, w * len(sides) + n, device)
            copy.start()
            edge_copies.append(copy)

    for w in range(wins):
        window(w)
        send_pieces(w)
        if w >= 2:
            sum_pieces(w - 2)

    grad_w = [dot(gp[c], xs[...], TN) for c in range(3)] + [dot(gp[3], gs[...], TN)]
    rows_w = 4 * inner
    part_w = rows_w // 2
    for c in range(4):
        first = c * inner
        w_core[first // part_w, first % part_w:first % part_w + inner, :] = grad_w[c].astype(BF16)
    count_w = [0]
    w_copies = []

    def post_w(src, dst, device):
        copy = remote(src, dst, w_sem, count_w[0], device)
        count_w[0] += 1
        copy.start()
        w_copies.append(copy)
        return copy

    keep = lax.rem(lat, 2)
    core_mate = rows_up[0]
    swap = post_w(w_core.at[1 - keep], w_core_in, core_mate)

    low_sum = jnp.zeros((block, lanes), F32)
    high_sum = jnp.zeros((block, lanes), F32)
    for b in range(WIN_LON):
        got = jnp.concatenate(
            [
                jnp.concatenate([gbias[t, (z * WIN_LON + b) * half:(z * WIN_LON + b + 1) * half, :] for t in range(tiles)], axis=1)
                for z in range(WIN_LEVEL)
            ],
            axis=0,
        )
        right = WIN_LAT * (WIN_LON - 1 - b)
        low_sum = low_sum + pltpu.roll(jnp.where(place <= b, got, 0.0), right, 1)
        high_sum = high_sum + pltpu.roll(jnp.where(place > b, got, 0.0), lanes - WIN_LAT * (b + 1), 1)

    swap.wait_recv()
    sub = part_w // 2
    orders = [
        [(b, m) for b, m in zip(lon_bits, mates)] + [(b, m) for b, m in zip(lat_bits[1:], rows_up[1:])],
        [(b, m) for b, m in zip(lat_bits[1:], rows_up[1:])] + [(b, m) for b, m in zip(lon_bits, mates)],
    ]
    steps = len(orders[0])
    flying = [None, None]
    for j in range(2):
        part = slice(j * sub, (j + 1) * sub)
        w_cur[0, j] = (w_core[keep, part, :].astype(F32) + w_core_in[part, :].astype(F32)).astype(BF16)
        flying[j] = post_w(w_cur.at[0, j], w_in.at[0, j], orders[j][0][1])

    gap = jnp.zeros((block, 128 - SIDE), F32)
    sums = jnp.concatenate(
        [
            jnp.concatenate(
                [low_sum[:, s * SIDE:(s + 1) * SIDE], gap, high_sum[:, s * SIDE:(s + 1) * SIDE], gap], axis=1
            )
            for s in range(segs)
        ],
        axis=0,
    ).astype(BF16)
    parts[:, :PART] = dot(sums, perm, NT)
    for k, h, r, c in spots:
        line[h * wins:(h + 1) * wins, k * SPAN:(k + 1) * SPAN] = parts[r:r + wins, c:c + SPAN]
    used = lax.broadcasted_iota(jnp.int32, line.shape, 0) < heads * wins
    inside = lax.broadcasted_iota(jnp.int32, line.shape, 1) < table.shape[2]
    bias_cur[0] = jnp.where(used & inside, line[...], 0.0).astype(BF16)
    count_b = [0]
    bias_copies = []

    def post_b(src, dst, device):
        copy = remote(src, dst, bias_sem, count_b[0], device)
        count_b[0] += 1
        copy.start()
        bias_copies.append(copy)
        return copy

    bias_step = post_b(bias_cur.at[0], bias_in.at[0], mates[0])

    for w in range(max(wins - 2, 0), wins):
        if w == wins - 1:
            break
        sum_pieces(w)

    def w_step(k):
        for j in range(2):
            flying[j].wait_recv()
            fresh = (w_cur[k, j].astype(F32) + w_in[k, j].astype(F32)).astype(BF16)
            w_cur[k + 1, j] = fresh
            if k + 1 < steps:
                flying[j] = post_w(w_cur.at[k + 1, j], w_in.at[k + 1, j], orders[j][k + 1][1])

    def bias_sum(k):
        bias_copies[k].wait_recv()
        fresh = bias_cur[k].astype(F32) + bias_in[k].astype(F32)
        if k + 1 < len(lon_bits):
            bias_cur[k + 1] = fresh.astype(BF16)
            post_b(bias_cur.at[k + 1], bias_in.at[k + 1], mates[k + 1])
        else:
            kind_row = lax.broadcasted_iota(jnp.int32, line.shape, 0) % wins
            kind = jnp.zeros(line.shape, F32)
            for w in range(wins):
                kind = jnp.where(kind_row == w, type_ref[0, w].astype(F32), kind)
            bias_cur[k + 1] = jnp.where(inside, fresh, kind).astype(BF16)
            all_bias_ref[pl.ds(lat, 1)] = bias_cur[k + 1][None]

    for k in range(len(lon_bits)):
        bias_sum(k)
    final = bias_cur.at[len(lon_bits)]
    spread_copies = []
    have = [lat]
    order = list(reversed(list(zip(lat_bits, rows_up))))
    for i, (b, device) in enumerate(order):
        for slot in have:
            src = final if slot is lat else all_bias_ref.at[slot]
            spread_copies.append(post_b(src, all_bias_ref.at[slot], device))
        have = have + [flip(slot, b) for slot in have]
        if i == 0:
            w_step(0)
            sum_pieces(wins - 1)
        if i + 1 < len(order):
            for copy in spread_copies:
                copy.wait_recv()
            spread_copies = []
    for k in range(1, steps):
        w_step(k)
    both_w = [
        post_w(w_cur.at[steps, j], all_w_ref.at[keep, pl.ds(j * sub, sub)], core_mate) for j in range(2)
    ]
    for j in range(2):
        all_w_ref[pl.ds(keep, 1), j * sub:(j + 1) * sub, :] = w_cur[steps, j][None]
    for copy in both_w + spread_copies + edge_copies:
        copy.wait_recv()
    for copy in sent + piece_copies + edge_copies + w_copies + bias_copies:
        copy.wait_send()


def block_backward(x, g, aw, ow, table, types, shift):
    lats_in, cols, levels, width = x.shape
    inner = aw.shape[1]
    heads, _, rel_total = table.shape
    lons, lats, groups = (lax.axis_size(name) for name in ("lon", "lat", "head"))
    wins = levels // WIN_LEVEL
    sides = 1 if lons <= 2 else 2
    lanes = up(heads * TOK, 128)
    tiles = lanes // 128
    block = WIN_LEVEL * WIN_LAT * wins
    rows = up(heads * wins, 16)
    long = up(rel_total + 1, 128)
    lon_steps = len(bits_of(lons))
    steps = lon_steps + len(bits_of(lats)) - 1
    packed = up(MAIN, 16)
    vmem = pl.BlockSpec(memory_space=pltpu.VMEM)
    smem = pl.BlockSpec(memory_space=pltpu.SMEM)
    hbm = pl.BlockSpec(memory_space=pltpu.HBM)
    dma = pltpu.SemaphoreType.DMA
    return pl.pallas_call(
        functools.partial(block_kernel, heads),
        out_shape=(
            pltpu.VMEM((wins, TOK, inner), BF16),
            pltpu.VMEM((sides, wins, 2 * EDGE, inner), BF16),
            pltpu.VMEM((2, 2 * inner, width), BF16),
            pltpu.VMEM((lats, rows, long), BF16),
        ),
        in_specs=[smem, smem] + [hbm] * 5,
        out_specs=(vmem,) * 4,
        scratch_shapes=[
            pltpu.VMEM(x.shape, BF16),
            pltpu.VMEM(g.shape, BF16),
            pltpu.VMEM(aw.shape, BF16),
            pltpu.VMEM(ow.shape, BF16),
            pltpu.VMEM(table.shape, F32),
            pltpu.VMEM((2, width // 128, EDGE * levels, 128), F32),
            pltpu.VMEM((2, width // 128, SIDE * levels, 128), F32),
            pltpu.VMEM((sides, wins, 4 * EDGE, width), BF16),
            pltpu.VMEM((sides, wins, 4 * EDGE, width), BF16),
            pltpu.VMEM((wins * TOK, width), BF16),
            pltpu.VMEM((wins * TOK, width), BF16),
            pltpu.VMEM((rows, long), F32),
            pltpu.VMEM((heads * WIN_LEVEL * block, 256), F32),
            pltpu.VMEM((tiles, TOK * wins, 128), F32),
            pltpu.VMEM((tiles, TOK * wins, 128), F32),
            pltpu.VMEM((4, wins * TOK, inner), BF16),
            pltpu.VMEM((3, inner, groups * 128), BF16),
            pltpu.VMEM((wins, groups, packed, 128), BF16),
            pltpu.VMEM((wins, groups - 1, packed, 128), BF16),
            pltpu.VMEM((sides, wins, 2 * EDGE, inner), BF16),
            pltpu.VMEM((2, 2 * inner, width), BF16),
            pltpu.VMEM((2 * inner, width), BF16),
            pltpu.VMEM((steps + 1, 2, inner, width), BF16),
            pltpu.VMEM((steps, 2, inner, width), BF16),
            pltpu.VMEM((lon_steps + 1, rows, long), BF16),
            pltpu.VMEM((lon_steps, rows, long), BF16),
            dma((5,)),
            dma((2, wins * sides)),
            dma((2, wins * (groups - 1))),
            dma((2, wins * sides)),
            dma((2, 2 * steps + 3)),
            dma((2, lon_steps + lats - 1)),
        ],
        compiler_params=pltpu.CompilerParams(
            collective_id=0, has_side_effects=True, vmem_limit_bytes=54 * 1024 * 1024
        ),
        cost_estimate=pl.CostEstimate(flops=10**9, bytes_accessed=10**7, transcendentals=10**6),
    )(shift, types, x, g, aw, ow, table)


def finish_kernel(lons, shift_ref, own_ref, edge_ref, w_ref, bias_ref,
                  feature_ref, aw_ref, ow_ref, table_ref, wide, edges):
    shift = shift_ref[0]
    early = shift <= HALF
    wins = own_ref.shape[0]
    chunk = own_ref.shape[2]
    levels = wins * WIN_LEVEL
    sides = edge_ref.shape[0]
    for w in range(wins):
        full = own_ref[w].astype(F32)
        if sides == 1:
            rim = edge_ref[0, w].astype(F32)
        else:
            rim = jnp.where(early, edge_ref[0, w].astype(F32), edge_ref[1, w].astype(F32))
        for z in range(WIN_LEVEL):
            level = WIN_LEVEL * w + z
            wide[pl.ds(level, SIDE, stride=levels), :chunk] = full[z * SIDE:(z + 1) * SIDE]
            edges[pl.ds(level, EDGE, stride=levels), :chunk] = rim[z * EDGE:(z + 1) * EDGE]
    run = WIN_LAT * levels
    for c in range(WIN_LON):
        here = lax.rem(c + WIN_LON - shift, WIN_LON)
        there = jnp.where(early, jnp.maximum(HALF + c - shift, 0), jnp.maximum(c - shift, 0))
        there = jnp.minimum(there, HALF - 1)
        flag = jnp.where(early, (c >= shift).astype(F32), (c < shift).astype(F32))
        near = wide[pl.ds(pl.multiple_of(here * run, 8), run), :]
        far = edges[pl.ds(pl.multiple_of(there * run, 8), run), :]
        mixed = near * flag + far * (1.0 - flag)
        feature_ref[:, c] = mixed.reshape(WIN_LAT, levels, 128)[:, :, :chunk].astype(BF16)
    inner = aw_ref.shape[1]
    flat = w_ref[...].reshape(4 * inner, w_ref.shape[2])
    for c in range(3):
        aw_ref[c] = flat[c * inner:(c + 1) * inner].astype(F32)
    ow_ref[...] = flat[3 * inner:].astype(F32)

    heads, types, total = table_ref.shape
    lats, rows, long = bias_ref.shape
    lines = bias_ref[...].reshape(lats * rows, long)
    kinds = lines[:, total:total + 1].astype(F32)
    held = lax.broadcasted_iota(jnp.int32, (lats * rows, types), 0) % rows // wins
    kind = lax.broadcasted_iota(jnp.int32, (lats * rows, types), 1).astype(F32)
    for h in range(heads):
        pick = jnp.where((kinds == kind) & (held == h), 1.0, 0.0).astype(BF16)
        table_ref[h] = dot(pick, lines, TN)[:, :total]


def finish(own, edge, all_w, all_bias, shift, types, heads, rel_total):
    wins, _, chunk = own.shape
    inner = all_w.shape[1] // 2
    levels = wins * WIN_LEVEL
    vmem = pl.BlockSpec(memory_space=pltpu.VMEM)
    return pl.pallas_call(
        functools.partial(finish_kernel, lax.axis_size("lon")),
        out_shape=(
            jax.ShapeDtypeStruct((WIN_LAT, WIN_LON, levels, chunk), BF16),
            jax.ShapeDtypeStruct((3, inner, all_w.shape[2]), F32),
            jax.ShapeDtypeStruct((inner, all_w.shape[2]), F32),
            jax.ShapeDtypeStruct((heads, types, rel_total), F32),
        ),
        in_specs=[pl.BlockSpec(memory_space=pltpu.SMEM)] + [vmem] * 4,
        out_specs=(vmem,) * 4,
        scratch_shapes=[
            pltpu.VMEM((SIDE * levels, 128), F32),
            pltpu.VMEM((EDGE * levels, 128), F32),
        ],
        compiler_params=pltpu.CompilerParams(vmem_limit_bytes=20 * 1024 * 1024),
    )(shift, own, edge, all_w, all_bias)


def per_device(features, attend_weight, output_weight, bias_table, bias_type, window_shift, grad_out):
    x, g = (v.transpose(1, 2, 0, 3) for v in (features, grad_out))
    aw = attend_weight.transpose(0, 2, 1)
    table = bias_table.transpose(1, 0, 2)
    gathered = block_backward(x, g, aw, output_weight, table, bias_type.T, window_shift)
    types, heads, rel_total = bias_table.shape
    feature_grad, attend_grad, output_grad, bias_grad = finish(*gathered, window_shift, types, heads, rel_total)
    return (
        feature_grad.transpose(2, 0, 1, 3),
        attend_grad.transpose(0, 2, 1),
        output_grad,
        bias_grad.transpose(1, 0, 2),
    )


def solution(mesh):
    placed = (
        P(None, "lat", "lon", None),
        P(None, None, "head"),
        P("head", None),
        P(None, "head", None),
        P(None, "lat"),
        P(),
        P(None, "lat", "lon", None),
    )
    return jax.shard_map(
        per_device,
        mesh=mesh,
        in_specs=placed,
        out_specs=(
            P(None, "lat", "lon", "head"),
            P(None, None, "head"),
            P("head", None),
            P(None, "head", None),
        ),
        check_vma=False,
    )
```

```python
import functools

import jax
import jax.numpy as jnp
from jax import lax
from jax.experimental import pallas as pl
from jax.experimental.pallas import tpu as pltpu
from jax.sharding import PartitionSpec as P

WIN_LEVEL = 2
WIN_LAT = 6
WIN_LON = 12
HALF = WIN_LON // 2
SPAN = 2 * WIN_LON - 1
SIDE = WIN_LON * WIN_LAT
TOK = WIN_LEVEL * SIDE
EDGE = HALF * WIN_LAT
MAIN = TOK - EDGE
PART = WIN_LAT * SPAN
LOG2E = 1.4426950408889634
F32 = jnp.float32
BF16 = jnp.bfloat16

NN = ((1,), (0,))
NT = ((1,), (1,))
TN = ((0,), (0,))


def dot(a, b, dims):
    return lax.dot_general(a, b, (dims, ((), ())), preferred_element_type=F32)


def up(n, to):
    return -(-n // to) * to


def bits_of(n):
    return [1 << k for k in range(n.bit_length() - 1)]


def flip(i, bit):
    return i + bit - 2 * bit * lax.rem(i // bit, 2)


def permutation():
    row = lax.broadcasted_iota(jnp.int32, (PART, 256), 0)
    out = lax.broadcasted_iota(jnp.int32, (PART, 256), 1)
    a, d = row // SPAN, row % SPAN
    place = jnp.where(d < WIN_LON, d * WIN_LAT + a, 128 + (d - WIN_LON) * WIN_LAT + a)
    return jnp.where(place == out, 1.0, 0.0).astype(BF16)


def back_permutation(lanes):
    row = lax.broadcasted_iota(jnp.int32, (256, lanes), 0)
    out = lax.broadcasted_iota(jnp.int32, (256, lanes), 1)
    at = row % 128
    d = at // WIN_LAT + jnp.where(row >= 128, WIN_LON, 0)
    hit = (at % WIN_LAT * PART + d == out) & (at < SIDE) & (d < SPAN)
    return jnp.where(hit, 1.0, 0.0).astype(BF16)


def lane_lon(lanes):
    return lax.broadcasted_iota(jnp.int32, (1, lanes), 1) % SIDE // WIN_LAT


def block_kernel(heads, shift_ref, type_ref, x_hbm, g_hbm, aw_hbm, ow_hbm, table_hbm,
                 own_ref, edge_ref, all_w_ref, all_bias_ref,
                 x_own, g_own, aw, ow, table, halo_f, own_f, halo_out, halo_in, xs, gs,
                 line, parts, bias, gbias, gp, aw_split, piece_out, piece_in, edge_out,
                 w_core, w_core_in, w_cur, w_in, bias_cur, bias_in, folds, spots_f, rows_f,
                 local, halo_sem, piece_sem, edge_sem, w_sem, bias_sem):
    lons, lats, groups = (lax.axis_size(name) for name in ("lon", "lat", "head"))
    lon, lat, head = (lax.axis_index(name) for name in ("lon", "lat", "head"))
    shift = shift_ref[0]
    early = shift <= HALF
    cols, levels, width = x_own.shape[1:]
    wins = levels // WIN_LEVEL
    inner = aw.shape[1]
    size = inner // heads
    total = heads * TOK
    lanes = up(total, 128)
    tiles = lanes // 128

    loads = [
        pltpu.make_async_copy(src, dst, local.at[i])
        for i, (src, dst) in enumerate(
            ((x_hbm, x_own), (g_hbm, g_own), (table_hbm, table), (aw_hbm, aw), (ow_hbm, ow))
        )
    ]
    for load in loads:
        load.start()

    east = (lax.rem(lon + 1, lons), lat, head)
    west = (lax.rem(lon + lons - 1, lons), lat, head)
    lon_bits, lat_bits = bits_of(lons), bits_of(lats)
    mates = [(flip(lon, b), lat, head) for b in lon_bits]
    rows_up = [(lon, flip(lat, b), head) for b in lat_bits]
    sides = [east] if lons <= 2 else [east, west]
    peers = [(lon, lat, lax.rem(head + n, groups)) for n in range(1, groups)]
    greet = sides + (mates if lons > 2 else []) + rows_up + peers
    barrier = pltpu.get_barrier_semaphore()
    for device in greet:
        pl.semaphore_signal(barrier, inc=1, device_id=device, device_id_type=pl.DeviceIdType.MESH)

    def remote(src, dst, sems, k, device):
        return pltpu.make_async_remote_copy(
            src_ref=src, dst_ref=dst, send_sem=sems.at[0, k], recv_sem=sems.at[1, k],
            device_id=device, device_id_type=pl.DeviceIdType.MESH,
        )

    strips = width // 128

    def put(dst, i, spot, value):
        value = value.astype(F32)
        for t in range(strips):
            dst[i, t, spot * levels:(spot + 1) * levels, :] = value[:, t * 128:(t + 1) * 128]

    def take(src, i, level, count):
        rows = pl.ds(level, count, stride=levels)
        return jnp.concatenate([src[i, t, rows, :] for t in range(strips)], axis=1)

    loads[0].wait()
    loads[1].wait()
    sent = []
    for n in range(len(sides)):
        for i, src in enumerate((x_own, g_own)):
            for b in range(HALF):
                low = jnp.maximum(shift + b - HALF, 0)
                high = jnp.minimum(shift + b, cols - 1)
                if lons <= 2:
                    col = jnp.where(early, low, high)
                else:
                    col = high if n == 0 else low
                for a in range(WIN_LAT):
                    put(halo_f, i, b * WIN_LAT + a, src[a, col])
        for w in range(wins):
            for i in range(2):
                rows = [take(halo_f, i, WIN_LEVEL * w + z, EDGE) for z in range(WIN_LEVEL)]
                halo_out[n, w, i * 2 * EDGE:(i + 1) * 2 * EDGE, :] = jnp.concatenate(rows, axis=0).astype(BF16)
    pl.semaphore_wait(barrier, len(greet))
    for w in range(wins):
        for n, device in enumerate(sides):
            copy = remote(halo_out.at[n, w], halo_in.at[n, w], halo_sem, w * len(sides) + n, device)
            copy.start()
            sent.append(copy)

    for i, src in enumerate((x_own, g_own)):
        for b in range(WIN_LON):
            col = jnp.where(early, jnp.minimum(shift + b, cols - 1), jnp.maximum(shift + b - WIN_LON, 0))
            for a in range(WIN_LAT):
                put(own_f, i, b * WIN_LAT + a, src[a, col])

    loads[2].wait()
    parts[...] = jnp.zeros_like(parts)
    for h in range(heads):
        for w in range(wins):
            line[h * wins + w:h * wins + w + 1, :table.shape[2]] = table[h, pl.ds(type_ref[0, w], 1), :]
    block = WIN_LEVEL * WIN_LAT * wins
    spots = []
    for k in range(WIN_LEVEL * WIN_LEVEL * WIN_LAT * WIN_LAT):
        zi, zj = k // (WIN_LEVEL * WIN_LAT * WIN_LAT), k // (WIN_LAT * WIN_LAT) % WIN_LEVEL
        ai, aj = k // WIN_LAT % WIN_LAT, k % WIN_LAT
        for h in range(heads):
            seg = h * WIN_LEVEL + zi
            spots.append((k, h, seg * block + (zj * WIN_LAT + aj) * wins, ai * SPAN))
    for k, h, r, c in spots:
        parts[r:r + wins, c:c + SPAN] = line[h * wins:(h + 1) * wins, k * SPAN:(k + 1) * SPAN]
    perm = permutation()
    flat = parts[:, :PART]
    one = flat.astype(BF16)
    rest = flat - one.astype(F32)
    two = rest.astype(BF16)
    three = (rest - two.astype(F32)).astype(BF16)
    spread = (dot(one, perm, NN) + dot(two, perm, NN) + dot(three, perm, NN)) * LOG2E
    segs = heads * WIN_LEVEL
    pad = jnp.zeros((block, lanes - total), F32)

    def gathered(start):
        pieces = [spread[s * block:(s + 1) * block, start:start + SIDE] for s in range(segs)]
        return jnp.concatenate(pieces + [pad], axis=1)

    lower, upper = gathered(0), gathered(128)
    place = lane_lon(lanes)
    half = WIN_LAT * wins
    for b in range(WIN_LON):
        left = (lanes - WIN_LAT * (WIN_LON - 1 - b)) % lanes
        both = jnp.where(
            place <= b, pltpu.roll(lower, left, 1), pltpu.roll(upper, WIN_LAT * (b + 1), 1)
        )
        for z in range(WIN_LEVEL):
            r = (z * WIN_LON + b) * half
            for t in range(tiles):
                bias[t, r:r + half, :] = both[z * half:(z + 1) * half, t * 128:(t + 1) * 128]

    loads[3].wait()
    loads[4].wait()
    for c in range(3):
        for g in range(groups):
            chunk = aw[c, :, g * inner:(g + 1) * inner]
            aw_split[c, :, g * 128:(g + 1) * 128] = jnp.concatenate(
                [chunk, jnp.zeros((inner, 128 - inner), BF16)], axis=1
            )

    key_lon = lax.broadcasted_iota(jnp.int32, (TOK, 1), 0) % SIDE // WIN_LAT
    mine = jnp.where(early, (key_lon + shift < WIN_LON).astype(F32), (key_lon + shift >= WIN_LON).astype(F32)) > 0.5
    diag = (
        lax.broadcasted_iota(jnp.int32, (inner, lanes), 0) // size
        == lax.broadcasted_iota(jnp.int32, (inner, lanes), 1) // TOK
    )
    col_head = lax.broadcasted_iota(jnp.int32, (TOK, inner), 1) // size
    scaling = size ** -0.5

    def expanded(rows):
        rows = rows.astype(BF16).astype(F32)
        filled = jnp.concatenate([rows] * heads + [jnp.zeros((inner, lanes - total), F32)], axis=1)
        return jnp.where(diag, filled, 0.0).astype(BF16)

    def folded(wide_rows):
        out = jnp.zeros((TOK, inner), F32)
        for h in range(heads):
            out = jnp.where(col_head == h, wide_rows[h * TOK:(h + 1) * TOK], out)
        return out

    piece_copies = []

    def window(w):
        span = slice(w * TOK, (w + 1) * TOK)
        for n in range(len(sides)):
            sent[w * len(sides) + n].wait_recv()
        for i, dst in enumerate((xs, gs)):
            kept = [take(own_f, i, WIN_LEVEL * w + z, SIDE) for z in range(WIN_LEVEL)]
            kept = jnp.concatenate(kept, axis=0)
            near = [halo_in[n, w, i * 2 * EDGE:(i + 1) * 2 * EDGE, :].astype(F32) for n in range(len(sides))]
            first, last = (near[0], near[0]) if lons <= 2 else (near[0], near[1])
            filled = jnp.concatenate([first[:EDGE], last[:EDGE], first[EDGE:], last[EDGE:]], axis=0)
            dst[span, :] = jnp.where(mine, kept, filled).astype(BF16)
        tokens, grads = xs[span, :], gs[span, :]
        queries = expanded(dot(aw[0], tokens, NT))
        keys = dot(tokens, aw[1], NT).astype(BF16)
        values = dot(tokens, aw[2], NT).astype(BF16)
        gates = expanded(dot(ow[...], grads, NT))
        rows = pl.ds(w, TOK, stride=wins)
        offset = jnp.concatenate([bias[t, rows, :] for t in range(tiles)], axis=1)
        scores = dot(keys, queries, NN) * (scaling * LOG2E) + offset
        top = jnp.max(scores, axis=0, keepdims=True)
        raised = jnp.exp2(scores - top)
        soft = raised * (1.0 / jnp.sum(raised, axis=0, keepdims=True))
        soft_half = soft.astype(BF16)
        both = soft * dot(values, gates, NN)
        slopes = both - soft * jnp.sum(both, axis=0, keepdims=True)
        for t in range(tiles):
            gbias[t, rows, :] = slopes[:, t * 128:(t + 1) * 128]
        slopes_half = slopes.astype(BF16)
        gp[0, span, :] = (folded(dot(slopes_half, keys, TN)) * scaling).astype(BF16)
        gp[1, span, :] = (dot(slopes_half, queries, NT) * scaling).astype(BF16)
        gp[2, span, :] = dot(soft_half, gates, NT).astype(BF16)
        gp[3, span, :] = folded(dot(soft_half, values, TN)).astype(BF16)

    def send_pieces(w):
        span = slice(w * TOK, (w + 1) * TOK)
        out = sum(dot(gp[c, span, :], aw_split[c], NN) for c in range(3))
        for g in range(groups):
            chunk = out[:, g * 128:g * 128 + inner]
            tail = chunk[MAIN:]
            third = 128 - inner
            extra = jnp.concatenate([tail[:, t * third:(t + 1) * third] for t in range(inner // third)], axis=0)
            packed = jnp.concatenate([chunk[:MAIN], extra], axis=1).astype(BF16)
            piece_out[w, g, :MAIN, :] = packed
        for n, device in enumerate(peers):
            copy = remote(
                piece_out.at[w, device[2]], piece_in.at[w, n], piece_sem, w * len(peers) + n, device
            )
            copy.start()
            piece_copies.append(copy)

    edge_copies = []

    def sum_pieces(w):
        for n in range(len(peers)):
            piece_copies[w * len(peers) + n].wait_recv()
        got = piece_out[w, head].astype(F32)
        for n in range(len(peers)):
            got = got + piece_in[w, n].astype(F32)
        third = 128 - inner
        tail = [got[t * EDGE:(t + 1) * EDGE, inner:] for t in range(inner // third)]
        full = jnp.concatenate([got[:MAIN, :inner], jnp.concatenate(tail, axis=1)], axis=0)
        own_ref[w] = full.astype(BF16)
        first = jnp.concatenate([full[:EDGE], full[SIDE:SIDE + EDGE]], axis=0)
        last = jnp.concatenate([full[EDGE:SIDE], full[SIDE + EDGE:]], axis=0)
        if lons <= 2:
            outs = [jnp.where(early, last, first)]
        else:
            outs = [last, first]
        for n, device in enumerate(sides):
            edge_out[n, w] = outs[n].astype(BF16)
            copy = remote(edge_out.at[n, w], edge_ref.at[n, w], edge_sem, w * len(sides) + n, device)
            copy.start()
            edge_copies.append(copy)

    strip_b = bias_cur.shape[2]
    back = back_permutation(rows_f.shape[0] * 128)
    folds[...] = jnp.zeros_like(folds)
    count_b = [0]
    bias_copies = []

    def post_b(src, dst, device):
        copy = remote(src, dst, bias_sem, count_b[0], device)
        count_b[0] += 1
        copy.start()
        bias_copies.append(copy)
        return copy

    def bias_line(w):
        for z in range(WIN_LEVEL):
            low = jnp.zeros((WIN_LAT, lanes), F32)
            high = jnp.zeros((WIN_LAT, lanes), F32)
            for b in range(WIN_LON):
                rows = pl.ds((z * WIN_LON + b) * half + w, WIN_LAT, stride=wins)
                got = jnp.concatenate([gbias[t, rows, :] for t in range(tiles)], axis=1)
                right = WIN_LAT * (WIN_LON - 1 - b)
                low = low + pltpu.roll(jnp.where(place <= b, got, 0.0), right, 1)
                high = high + pltpu.roll(jnp.where(place > b, got, 0.0), lanes - WIN_LAT * (b + 1), 1)
            for g in range(segs):
                r = (g * WIN_LEVEL + z) * 8
                folds[r:r + WIN_LAT, :SIDE] = low[:, g * SIDE:(g + 1) * SIDE]
                folds[r:r + WIN_LAT, 128:128 + SIDE] = high[:, g * SIDE:(g + 1) * SIDE]
        spread_out = dot(folds[...].astype(BF16), back, NN)
        count = segs * WIN_LEVEL
        for t in range(spots_f.shape[0]):
            spots_f[t] = spread_out[:, t * 128:(t + 1) * 128]
        sums = jnp.zeros((count, spots_f.shape[0] * 128), F32)
        for a in range(WIN_LAT):
            rows = pl.ds(a, count, stride=8)
            got = jnp.concatenate([spots_f[t, rows, :] for t in range(spots_f.shape[0])], axis=1)
            sums = sums + (pltpu.roll(got, a * SPAN, 1) if a else got)
        for t in range(rows_f.shape[0]):
            rows_f[t, :count, :] = sums[:, t * 128:(t + 1) * 128]
        quarters = WIN_LEVEL * WIN_LEVEL
        run = WIN_LAT * PART
        found = []
        for q in range(quarters):
            rows = pl.ds(q, heads, stride=quarters)
            found.append(jnp.concatenate([rows_f[t, rows, :] for t in range(rows_f.shape[0])], axis=1)[:, :run])
        found.append(jnp.zeros((heads, 2 * strip_b - quarters * run), F32))
        full = jnp.concatenate(found, axis=1)
        both = [full[:, :strip_b], full[:, strip_b:], jnp.zeros((8 - 2 * heads, strip_b), F32)]
        bias_cur[0, w * 8:(w + 1) * 8, :] = jnp.concatenate(both, axis=0).astype(BF16)
        return post_b(bias_cur.at[0, pl.ds(w * 8, 8)], bias_in.at[0, pl.ds(w * 8, 8)], mates[0])

    lon_steps = len(lon_bits)

    def bias_total(first, last, flights):
        rows, span = slice(first * 8, last * 8), pl.ds(first * 8, (last - first) * 8)
        for k in range(lon_steps):
            for copy in flights:
                copy.wait_recv()
            fresh = bias_cur[k, rows, :].astype(F32) + bias_in[k, rows, :].astype(F32)
            if k + 1 == lon_steps:
                row = lax.broadcasted_iota(jnp.int32, fresh.shape, 0)
                for w in range(first, last):
                    fresh = jnp.where(row == (w - first) * 8 + 2 * heads, type_ref[0, w].astype(F32), fresh)
            bias_cur[k + 1, rows, :] = fresh.astype(BF16)
            if k + 1 < lon_steps:
                flights = [post_b(bias_cur.at[k + 1, span], bias_in.at[k + 1, span], mates[k + 1])]
        all_bias_ref[pl.ds(lat, 1), rows, :] = bias_cur[lon_steps, rows, :][None]
        return span

    gather_order = list(reversed(list(zip(lat_bits, rows_up))))

    def bias_gather(step, span, have, flights):
        for copy in flights:
            copy.wait_recv()
        bit, device = gather_order[step]
        out = []
        for slot in have:
            src = bias_cur.at[lon_steps, span] if slot is lat else all_bias_ref.at[slot, span]
            out.append(post_b(src, all_bias_ref.at[slot, span], device))
        return have + [flip(slot, bit) for slot in have], out

    lines = []
    for w in range(wins):
        window(w)
        send_pieces(w)
        if w < wins - 1:
            lines.append(bias_line(w))
        if w >= 2:
            sum_pieces(w - 2)

    grad_w = [dot(gp[c], xs[...], TN) for c in range(3)] + [dot(gp[3], gs[...], TN)]
    rows_w = 4 * inner
    part_w = rows_w // 2
    for c in range(4):
        first = c * inner
        w_core[first // part_w, first % part_w:first % part_w + inner, :] = grad_w[c].astype(BF16)
    count_w = [0]
    w_copies = []

    def post_w(src, dst, device):
        copy = remote(src, dst, w_sem, count_w[0], device)
        count_w[0] += 1
        copy.start()
        w_copies.append(copy)
        return copy

    keep = lax.rem(lat, 2)
    core_mate = rows_up[0]
    swap = post_w(w_core.at[1 - keep], w_core_in, core_mate)

    early_span = bias_total(0, wins - 1, lines)
    early_have, early_out = bias_gather(0, early_span, [lat], [])
    last_line = bias_line(wins - 1)

    swap.wait_recv()
    sub = part_w // 2
    orders = [
        [(b, m) for b, m in zip(lon_bits, mates)] + [(b, m) for b, m in zip(lat_bits[1:], rows_up[1:])],
        [(b, m) for b, m in zip(lat_bits[1:], rows_up[1:])] + [(b, m) for b, m in zip(lon_bits, mates)],
    ]
    steps = len(orders[0])
    flying = [None, None]
    for j in range(2):
        part = slice(j * sub, (j + 1) * sub)
        w_cur[0, j] = (w_core[keep, part, :].astype(F32) + w_core_in[part, :].astype(F32)).astype(BF16)
        flying[j] = post_w(w_cur.at[0, j], w_in.at[0, j], orders[j][0][1])

    for w in range(max(wins - 2, 0), wins - 1):
        sum_pieces(w)

    def w_step(k):
        for j in range(2):
            flying[j].wait_recv()
            fresh = (w_cur[k, j].astype(F32) + w_in[k, j].astype(F32)).astype(BF16)
            w_cur[k + 1, j] = fresh
            if k + 1 < steps:
                flying[j] = post_w(w_cur.at[k + 1, j], w_in.at[k + 1, j], orders[j][k + 1][1])

    late_have, late_out = [lat], []
    for i in range(len(gather_order)):
        if i + 1 < len(gather_order):
            early_have, early_out = bias_gather(i + 1, early_span, early_have, early_out)
        if i == 0:
            late_span = bias_total(wins - 1, wins, [last_line])
        late_have, late_out = bias_gather(i, late_span, late_have, late_out)
        if i == 0:
            w_step(0)
            sum_pieces(wins - 1)
    for k in range(1, steps):
        w_step(k)
    both_w = [
        post_w(w_cur.at[steps, j], all_w_ref.at[keep, pl.ds(j * sub, sub)], core_mate) for j in range(2)
    ]
    for j in range(2):
        all_w_ref[pl.ds(keep, 1), j * sub:(j + 1) * sub, :] = w_cur[steps, j][None]
    for copy in both_w + early_out + late_out + edge_copies:
        copy.wait_recv()
    for copy in sent + piece_copies + edge_copies + w_copies + bias_copies:
        copy.wait_send()


def block_backward(x, g, aw, ow, table, types, shift):
    lats_in, cols, levels, width = x.shape
    inner = aw.shape[1]
    heads, _, rel_total = table.shape
    lons, lats, groups = (lax.axis_size(name) for name in ("lon", "lat", "head"))
    wins = levels // WIN_LEVEL
    sides = 1 if lons <= 2 else 2
    lanes = up(heads * TOK, 128)
    tiles = lanes // 128
    block = WIN_LEVEL * WIN_LAT * wins
    rows = up(heads * wins, 16)
    long = up(rel_total + 1, 128)
    lon_steps = len(bits_of(lons))
    steps = lon_steps + len(bits_of(lats)) - 1
    packed = up(MAIN, 16)
    strip = up(rel_total, 256) // 2
    quads = heads * WIN_LEVEL * WIN_LEVEL
    vmem = pl.BlockSpec(memory_space=pltpu.VMEM)
    smem = pl.BlockSpec(memory_space=pltpu.SMEM)
    hbm = pl.BlockSpec(memory_space=pltpu.HBM)
    dma = pltpu.SemaphoreType.DMA
    return pl.pallas_call(
        functools.partial(block_kernel, heads),
        out_shape=(
            pltpu.VMEM((wins, TOK, inner), BF16),
            pltpu.VMEM((sides, wins, 2 * EDGE, inner), BF16),
            pltpu.VMEM((2, 2 * inner, width), BF16),
            pltpu.VMEM((lats, wins * 8, strip), BF16),
        ),
        in_specs=[smem, smem] + [hbm] * 5,
        out_specs=(vmem,) * 4,
        scratch_shapes=[
            pltpu.VMEM(x.shape, BF16),
            pltpu.VMEM(g.shape, BF16),
            pltpu.VMEM(aw.shape, BF16),
            pltpu.VMEM(ow.shape, BF16),
            pltpu.VMEM(table.shape, F32),
            pltpu.VMEM((2, width // 128, EDGE * levels, 128), F32),
            pltpu.VMEM((2, width // 128, SIDE * levels, 128), F32),
            pltpu.VMEM((sides, wins, 4 * EDGE, width), BF16),
            pltpu.VMEM((sides, wins, 4 * EDGE, width), BF16),
            pltpu.VMEM((wins * TOK, width), BF16),
            pltpu.VMEM((wins * TOK, width), BF16),
            pltpu.VMEM((rows, long), F32),
            pltpu.VMEM((heads * WIN_LEVEL * block, 256), F32),
            pltpu.VMEM((tiles, TOK * wins, 128), F32),
            pltpu.VMEM((tiles, TOK * wins, 128), F32),
            pltpu.VMEM((4, wins * TOK, inner), BF16),
            pltpu.VMEM((3, inner, groups * 128), BF16),
            pltpu.VMEM((wins, groups, packed, 128), BF16),
            pltpu.VMEM((wins, groups - 1, packed, 128), BF16),
            pltpu.VMEM((sides, wins, 2 * EDGE, inner), BF16),
            pltpu.VMEM((2, 2 * inner, width), BF16),
            pltpu.VMEM((2 * inner, width), BF16),
            pltpu.VMEM((steps + 1, 2, inner, width), BF16),
            pltpu.VMEM((steps, 2, inner, width), BF16),
            pltpu.VMEM((lon_steps + 1, wins * 8, strip), BF16),
            pltpu.VMEM((lon_steps, wins * 8, strip), BF16),
            pltpu.VMEM((quads * 8, 256), F32),
            pltpu.VMEM((up(WIN_LAT * PART, 128) // 128, quads * 8, 128), F32),
            pltpu.VMEM((up(WIN_LAT * PART, 128) // 128, up(quads, 8), 128), F32),
            dma((5,)),
            dma((2, wins * sides)),
            dma((2, wins * (groups - 1))),
            dma((2, wins * sides)),
            dma((2, 2 * steps + 3)),
            dma((2, wins + 2 * (lon_steps - 1) + 2 * (lats - 1))),
        ],
        compiler_params=pltpu.CompilerParams(
            collective_id=0, has_side_effects=True, vmem_limit_bytes=54 * 1024 * 1024
        ),
        cost_estimate=pl.CostEstimate(flops=10**9, bytes_accessed=10**7, transcendentals=10**6),
    )(shift, types, x, g, aw, ow, table)


def finish_kernel(shift_ref, own_ref, edge_ref, w_ref, bias_ref,
                  feature_out, aw_out, ow_out, table_out,
                  feature, aw, ow, table, wide, edges, sems):
    shift = shift_ref[0]
    early = shift <= HALF
    wins = own_ref.shape[0]
    chunk = own_ref.shape[2]
    levels = wins * WIN_LEVEL
    sides = edge_ref.shape[0]
    heads, types, total = table.shape
    lats, _, strip = bias_ref.shape
    copies = []

    def put(src, dst):
        copy = pltpu.make_async_copy(src, dst, sems.at[len(copies)])
        copy.start()
        copies.append(copy)

    count = lats * wins
    lines = bias_ref[...].reshape(count * 8, strip)
    kinds = lines[:, :128].astype(F32).reshape(count, 8, 128)[:, 2 * heads:2 * heads + 1, :types]
    kind = lax.broadcasted_iota(jnp.int32, (count, 8, types), 2).astype(F32)
    row = lax.broadcasted_iota(jnp.int32, (count, 8, types), 1)
    same = kinds == kind
    for h in range(heads):
        for p in range(2):
            pick = jnp.where(same & (row == p * heads + h), 1.0, 0.0).reshape(count * 8, types).astype(BF16)
            stop = min(total, (p + 1) * strip)
            table[h, :, p * strip:stop] = dot(pick, lines, TN)[:, :stop - p * strip]
        put(table.at[h], table_out.at[h])

    inner = aw.shape[1]
    flat = w_ref[...].reshape(4 * inner, w_ref.shape[2])
    for c in range(3):
        aw[c] = flat[c * inner:(c + 1) * inner].astype(F32)
    ow[...] = flat[3 * inner:].astype(F32)
    put(aw, aw_out)
    put(ow, ow_out)

    for w in range(wins):
        full = own_ref[w].astype(F32)
        if sides == 1:
            rim = edge_ref[0, w].astype(F32)
        else:
            rim = jnp.where(early, edge_ref[0, w].astype(F32), edge_ref[1, w].astype(F32))
        for z in range(WIN_LEVEL):
            level = WIN_LEVEL * w + z
            wide[pl.ds(level, SIDE, stride=levels), :chunk] = full[z * SIDE:(z + 1) * SIDE]
            edges[pl.ds(level, EDGE, stride=levels), :chunk] = rim[z * EDGE:(z + 1) * EDGE]
    run = WIN_LAT * levels
    for c in range(WIN_LON):
        here = lax.rem(c + WIN_LON - shift, WIN_LON)
        there = jnp.where(early, jnp.maximum(HALF + c - shift, 0), jnp.maximum(c - shift, 0))
        there = jnp.minimum(there, HALF - 1)
        local = jnp.where(early, (c >= shift).astype(F32), (c < shift).astype(F32)) > 0.5
        near = wide[pl.ds(pl.multiple_of(here * run, 8), run), :]
        far = edges[pl.ds(pl.multiple_of(there * run, 8), run), :]
        mixed = jnp.where(local, near, far)
        feature[:, c] = mixed.reshape(WIN_LAT, levels, 128)[:, :, :chunk].astype(BF16)
    put(feature, feature_out)
    for copy in copies:
        copy.wait()


def finish(own, edge, all_w, all_bias, shift, types, heads, rel_total):
    wins, _, chunk = own.shape
    inner = all_w.shape[1] // 2
    levels = wins * WIN_LEVEL
    vmem = pl.BlockSpec(memory_space=pltpu.VMEM)
    outs = (
        ((WIN_LAT, WIN_LON, levels, chunk), BF16),
        ((3, inner, all_w.shape[2]), F32),
        ((inner, all_w.shape[2]), F32),
        ((heads, types, rel_total), F32),
    )
    return pl.pallas_call(
        finish_kernel,
        out_shape=tuple(jax.ShapeDtypeStruct(*out) for out in outs),
        in_specs=[pl.BlockSpec(memory_space=pltpu.SMEM)] + [vmem] * 4,
        out_specs=(pl.BlockSpec(memory_space=pl.ANY),) * 4,
        scratch_shapes=[pltpu.VMEM(*out) for out in outs] + [
            pltpu.VMEM((SIDE * levels, 128), F32),
            pltpu.VMEM((EDGE * levels, 128), F32),
            pltpu.SemaphoreType.DMA((heads + 3,)),
        ],
        compiler_params=pltpu.CompilerParams(vmem_limit_bytes=20 * 1024 * 1024),
    )(shift, own, edge, all_w, all_bias)


def per_device(features, attend_weight, output_weight, bias_table, bias_type, window_shift, grad_out):
    x, g = (v.transpose(1, 2, 0, 3) for v in (features, grad_out))
    aw = attend_weight.transpose(0, 2, 1)
    table = bias_table.transpose(1, 0, 2)
    gathered = block_backward(x, g, aw, output_weight, table, bias_type.T, window_shift)
    types, heads, rel_total = bias_table.shape
    feature_grad, attend_grad, output_grad, bias_grad = finish(*gathered, window_shift, types, heads, rel_total)
    return (
        feature_grad.transpose(2, 0, 1, 3),
        attend_grad.transpose(0, 2, 1),
        output_grad,
        bias_grad.transpose(1, 0, 2),
    )


def solution(mesh):
    placed = (
        P(None, "lat", "lon", None),
        P(None, None, "head"),
        P("head", None),
        P(None, "head", None),
        P(None, "lat"),
        P(),
        P(None, "lat", "lon", None),
    )
    return jax.shard_map(
        per_device,
        mesh=mesh,
        in_specs=placed,
        out_specs=(
            P(None, "lat", "lon", "head"),
            P(None, None, "head"),
            P("head", None),
            P(None, "head", None),
        ),
        check_vma=False,
    )
```

```python
import functools

import jax
import jax.numpy as jnp
from jax import lax
from jax.experimental import pallas as pl
from jax.experimental.pallas import tpu as pltpu
from jax.sharding import PartitionSpec as P

WIN_LEVEL = 2
WIN_LAT = 6
WIN_LON = 12
HALF = WIN_LON // 2
SPAN = 2 * WIN_LON - 1
SIDE = WIN_LON * WIN_LAT
TOK = WIN_LEVEL * SIDE
EDGE = HALF * WIN_LAT
MAIN = TOK - EDGE
PART = WIN_LAT * SPAN
LOG2E = 1.4426950408889634
F32 = jnp.float32
BF16 = jnp.bfloat16

NN = ((1,), (0,))
NT = ((1,), (1,))
TN = ((0,), (0,))


def dot(a, b, dims):
    return lax.dot_general(a, b, (dims, ((), ())), preferred_element_type=F32)


def up(n, to):
    return -(-n // to) * to


def bits_of(n):
    return [1 << k for k in range(n.bit_length() - 1)]


def flip(i, bit):
    return i + bit - 2 * bit * lax.rem(i // bit, 2)


def permutation():
    row = lax.broadcasted_iota(jnp.int32, (PART, 256), 0)
    out = lax.broadcasted_iota(jnp.int32, (PART, 256), 1)
    a, d = row // SPAN, row % SPAN
    place = jnp.where(d < WIN_LON, d * WIN_LAT + a, 128 + (d - WIN_LON) * WIN_LAT + a)
    return jnp.where(place == out, 1.0, 0.0).astype(BF16)


def back_permutation(lanes):
    row = lax.broadcasted_iota(jnp.int32, (256, lanes), 0)
    out = lax.broadcasted_iota(jnp.int32, (256, lanes), 1)
    at = row % 128
    d = at // WIN_LAT + jnp.where(row >= 128, WIN_LON, 0)
    hit = (at % WIN_LAT * PART + d == out) & (at < SIDE) & (d < SPAN)
    return jnp.where(hit, 1.0, 0.0).astype(BF16)


def lane_lon(lanes):
    return lax.broadcasted_iota(jnp.int32, (1, lanes), 1) % SIDE // WIN_LAT


def tail_order(wins, steps, gathers):
    tasks = [("piece", w) for w in range(2, wins - 1)]
    tasks += [("w", 0), ("sum", 0), ("late", 0)] + [("early", i) for i in range(1, gathers)]
    tasks += [("piece", wins - 1)] + [("w", k) for k in range(1, steps)] + [("late", i) for i in range(1, gathers)]
    return tasks


def block_kernel(heads, reach, shift_ref, type_ref, x_hbm, g_hbm, aw_hbm, ow_hbm, table_hbm,
                 own_ref, edge_ref, all_w_ref, all_bias_ref,
                 x_own, g_own, aw, ow, table, halo_f, own_f, halo_out, halo_in, xs, gs,
                 line, parts, bias, gbias, gp, aw_split, piece_out, piece_in, edge_out,
                 w_core, w_core_in, w_cur, w_in, bias_cur, bias_in, w_acc, folds, spots_f, rows_f,
                 local, halo_sem, piece_sem, edge_sem, w_sem, bias_sem):
    lons, lats, groups = (lax.axis_size(name) for name in ("lon", "lat", "head"))
    lon, lat, head = (lax.axis_index(name) for name in ("lon", "lat", "head"))
    shift = shift_ref[0]
    early = shift <= HALF
    rim = reach * WIN_LAT
    cols, levels, width = x_own.shape[1:]
    wins = levels // WIN_LEVEL
    inner = aw.shape[1]
    size = inner // heads
    total = heads * TOK
    lanes = up(total, 128)
    tiles = lanes // 128

    loads = [
        pltpu.make_async_copy(src, dst, local.at[i])
        for i, (src, dst) in enumerate(
            ((x_hbm, x_own), (g_hbm, g_own), (table_hbm, table), (aw_hbm, aw), (ow_hbm, ow))
        )
    ]
    for load in loads:
        load.start()

    east = (lax.rem(lon + 1, lons), lat, head)
    west = (lax.rem(lon + lons - 1, lons), lat, head)
    lon_bits, lat_bits = bits_of(lons), bits_of(lats)
    mates = [(flip(lon, b), lat, head) for b in lon_bits]
    rows_up = [(lon, flip(lat, b), head) for b in lat_bits]
    sides = [east] if lons <= 2 else [east, west]
    peers = [(lon, lat, lax.rem(head + n, groups)) for n in range(1, groups)]
    greet = sides + (mates if lons > 2 else []) + rows_up + peers
    barrier = pltpu.get_barrier_semaphore()
    for device in greet:
        pl.semaphore_signal(barrier, inc=1, device_id=device, device_id_type=pl.DeviceIdType.MESH)

    def remote(src, dst, sems, k, device):
        return pltpu.make_async_remote_copy(
            src_ref=src, dst_ref=dst, send_sem=sems.at[0, k], recv_sem=sems.at[1, k],
            device_id=device, device_id_type=pl.DeviceIdType.MESH,
        )

    strips = width // 128

    def put(dst, i, spot, value):
        value = value.astype(F32)
        for t in range(strips):
            dst[i, t, spot * levels:(spot + 1) * levels, :] = value[:, t * 128:(t + 1) * 128]

    def take(src, i, level, count):
        rows = pl.ds(level, count, stride=levels)
        return jnp.concatenate([src[i, t, rows, :] for t in range(strips)], axis=1)

    loads[0].wait()
    loads[1].wait()
    sent = []
    for n in range(len(sides)):
        for i, src in enumerate((x_own, g_own)):
            for b in range(reach):
                low = jnp.maximum(shift + b - reach, 0)
                high = jnp.minimum(shift + b, cols - 1)
                if lons <= 2:
                    col = jnp.where(early, low, high)
                else:
                    col = high if n == 0 else low
                for a in range(WIN_LAT):
                    put(halo_f, i, b * WIN_LAT + a, src[a, col])
        for w in range(wins):
            rows = [take(halo_f, i, WIN_LEVEL * w + z, rim) for i in range(2) for z in range(WIN_LEVEL)]
            halo_out[n, w] = jnp.concatenate(rows, axis=0).astype(BF16)
    pl.semaphore_wait(barrier, len(greet))
    for w in range(wins):
        for n, device in enumerate(sides):
            copy = remote(halo_out.at[n, w], halo_in.at[n, w], halo_sem, w * len(sides) + n, device)
            copy.start()
            sent.append(copy)

    for i, src in enumerate((x_own, g_own)):
        for b in range(WIN_LON):
            col = jnp.where(early, jnp.minimum(shift + b, cols - 1), jnp.maximum(shift + b - WIN_LON, 0))
            for a in range(WIN_LAT):
                put(own_f, i, b * WIN_LAT + a, src[a, col])

    loads[2].wait()
    parts[...] = jnp.zeros_like(parts)
    for h in range(heads):
        for w in range(wins):
            line[h * wins + w:h * wins + w + 1, :table.shape[2]] = table[h, pl.ds(type_ref[0, w], 1), :]
    block = WIN_LEVEL * WIN_LAT * wins
    spots = []
    for k in range(WIN_LEVEL * WIN_LEVEL * WIN_LAT * WIN_LAT):
        zi, zj = k // (WIN_LEVEL * WIN_LAT * WIN_LAT), k // (WIN_LAT * WIN_LAT) % WIN_LEVEL
        ai, aj = k // WIN_LAT % WIN_LAT, k % WIN_LAT
        for h in range(heads):
            seg = h * WIN_LEVEL + zi
            spots.append((k, h, seg * block + (zj * WIN_LAT + aj) * wins, ai * SPAN))
    for k, h, r, c in spots:
        parts[r:r + wins, c:c + SPAN] = line[h * wins:(h + 1) * wins, k * SPAN:(k + 1) * SPAN]
    perm = permutation()
    flat = parts[:, :PART]
    one = flat.astype(BF16)
    rest = flat - one.astype(F32)
    two = rest.astype(BF16)
    three = (rest - two.astype(F32)).astype(BF16)
    spread = (dot(one, perm, NN) + dot(two, perm, NN) + dot(three, perm, NN)) * LOG2E
    segs = heads * WIN_LEVEL
    pad = jnp.zeros((block, lanes - total), F32)

    def gathered(start):
        pieces = [spread[s * block:(s + 1) * block, start:start + SIDE] for s in range(segs)]
        return jnp.concatenate(pieces + [pad], axis=1)

    lower, upper = gathered(0), gathered(128)
    place = lane_lon(lanes)
    half = WIN_LAT * wins
    for b in range(WIN_LON):
        left = (lanes - WIN_LAT * (WIN_LON - 1 - b)) % lanes
        both = jnp.where(
            place <= b, pltpu.roll(lower, left, 1), pltpu.roll(upper, WIN_LAT * (b + 1), 1)
        )
        for z in range(WIN_LEVEL):
            r = (z * WIN_LON + b) * half
            for t in range(tiles):
                bias[t, r:r + half, :] = both[z * half:(z + 1) * half, t * 128:(t + 1) * 128]

    loads[3].wait()
    loads[4].wait()
    gp[...] = jnp.zeros_like(gp)
    aw_split[...] = jnp.zeros_like(aw_split)
    for c in range(3):
        for g in range(groups):
            aw_split[c * 128:c * 128 + inner, g * 128:g * 128 + inner] = aw[c, :, g * inner:(g + 1) * inner]

    key_lon = lax.broadcasted_iota(jnp.int32, (TOK, 1), 0) % SIDE // WIN_LAT
    mine = jnp.where(early, (key_lon + shift < WIN_LON).astype(F32), (key_lon + shift >= WIN_LON).astype(F32)) > 0.5
    diag = (
        lax.broadcasted_iota(jnp.int32, (inner, lanes), 0) // size
        == lax.broadcasted_iota(jnp.int32, (inner, lanes), 1) // TOK
    )
    col_head = lax.broadcasted_iota(jnp.int32, (TOK, inner), 1) // size
    scaling = size ** -0.5

    def expanded(rows):
        rows = rows.astype(BF16).astype(F32)
        filled = jnp.concatenate([rows] * heads + [jnp.zeros((inner, lanes - total), F32)], axis=1)
        return jnp.where(diag, filled, 0.0).astype(BF16)

    def folded(wide_rows):
        out = jnp.zeros((TOK, inner), F32)
        for h in range(heads):
            out = jnp.where(col_head == h, wide_rows[h * TOK:(h + 1) * TOK], out)
        return out

    piece_copies = []

    def window(w):
        span = slice(w * TOK, (w + 1) * TOK)
        for n in range(len(sides)):
            sent[w * len(sides) + n].wait_recv()
        arrived = [halo_in[n, w].astype(F32) for n in range(len(sides))]
        for i, dst in enumerate((xs, gs)):
            kept = [take(own_f, i, WIN_LEVEL * w + z, SIDE) for z in range(WIN_LEVEL)]
            kept = jnp.concatenate(kept, axis=0)
            near = [got[i * 2 * rim:(i + 1) * 2 * rim] for got in arrived]
            first, last = near[0], near[-1]
            filled = []
            for z in range(WIN_LEVEL):
                part, start = slice(z * rim, (z + 1) * rim), z * SIDE
                filled += [first[part], kept[start + rim:start + SIDE - rim], last[part]]
            filled = jnp.concatenate([f for f in filled if f.shape[0]], axis=0)
            dst[span, :] = jnp.where(mine, kept, filled).astype(BF16)
        tokens, grads = xs[span, :], gs[span, :]
        queries = expanded(dot(aw[0], tokens, NT))
        keys = dot(tokens, aw[1], NT).astype(BF16)
        values = dot(tokens, aw[2], NT).astype(BF16)
        gates = expanded(dot(ow[...], grads, NT))
        rows = pl.ds(w, TOK, stride=wins)
        offset = jnp.concatenate([bias[t, rows, :] for t in range(tiles)], axis=1)
        scores = dot(keys, queries, NN) * (scaling * LOG2E) + offset
        top = jnp.max(scores, axis=0, keepdims=True)
        raised = jnp.exp2(scores - top)
        soft = raised * (1.0 / jnp.sum(raised, axis=0, keepdims=True))
        soft_half = soft.astype(BF16)
        both = soft * dot(values, gates, NN)
        slopes = both - soft * jnp.sum(both, axis=0, keepdims=True)
        for t in range(tiles):
            gbias[t, rows, :] = slopes[:, t * 128:(t + 1) * 128]
        slopes_half = slopes.astype(BF16)
        gp[span, 0 * 128:0 * 128 + inner] = (folded(dot(slopes_half, keys, TN)) * scaling).astype(BF16)
        gp[span, 1 * 128:1 * 128 + inner] = (dot(slopes_half, queries, NT) * scaling).astype(BF16)
        gp[span, 2 * 128:2 * 128 + inner] = dot(soft_half, gates, NT).astype(BF16)
        gp[span, 3 * 128:3 * 128 + inner] = folded(dot(soft_half, values, TN)).astype(BF16)

    def send_pieces(w):
        span = slice(w * TOK, (w + 1) * TOK)
        out = dot(gp[span, :3 * 128], aw_split[...], NN)
        for g in range(groups):
            chunk = out[:, g * 128:g * 128 + inner]
            tail = chunk[MAIN:]
            third = 128 - inner
            extra = jnp.concatenate([tail[:, t * third:(t + 1) * third] for t in range(inner // third)], axis=0)
            packed = jnp.concatenate([chunk[:MAIN], extra], axis=1).astype(BF16)
            piece_out[w, g, :MAIN, :] = packed
        for n, device in enumerate(peers):
            copy = remote(
                piece_out.at[w, device[2]], piece_in.at[w, n], piece_sem, w * len(peers) + n, device
            )
            copy.start()
            piece_copies.append(copy)

    edge_copies = []

    def sum_pieces(w):
        for n in range(len(peers)):
            piece_copies[w * len(peers) + n].wait_recv()
        got = piece_out[w, head].astype(F32)
        for n in range(len(peers)):
            got = got + piece_in[w, n].astype(F32)
        third = 128 - inner
        tail = [got[t * EDGE:(t + 1) * EDGE, inner:] for t in range(inner // third)]
        full = jnp.concatenate([got[:MAIN, :inner], jnp.concatenate(tail, axis=1)], axis=0)
        own_ref[w] = full.astype(BF16)
        first = jnp.concatenate([full[:rim], full[SIDE:SIDE + rim]], axis=0)
        last = jnp.concatenate([full[SIDE - rim:SIDE], full[2 * SIDE - rim:]], axis=0)
        if lons <= 2:
            outs = [jnp.where(early, last, first)]
        else:
            outs = [last, first]
        for n, device in enumerate(sides):
            edge_out[n, w] = outs[n].astype(BF16)
            copy = remote(edge_out.at[n, w], edge_ref.at[n, w], edge_sem, w * len(sides) + n, device)
            copy.start()
            edge_copies.append(copy)

    strip_b = bias_cur.shape[2]
    back = back_permutation(rows_f.shape[0] * 128)
    folds[...] = jnp.zeros_like(folds)
    count_b = [0]
    bias_copies = []

    def post_b(src, dst, device):
        copy = remote(src, dst, bias_sem, count_b[0], device)
        count_b[0] += 1
        copy.start()
        bias_copies.append(copy)
        return copy

    def bias_line(w):
        for z in range(WIN_LEVEL):
            low = jnp.zeros((WIN_LAT, lanes), F32)
            high = jnp.zeros((WIN_LAT, lanes), F32)
            for b in range(WIN_LON):
                rows = pl.ds((z * WIN_LON + b) * half + w, WIN_LAT, stride=wins)
                got = jnp.concatenate([gbias[t, rows, :] for t in range(tiles)], axis=1)
                right = WIN_LAT * (WIN_LON - 1 - b)
                if right == 0:
                    low = low + got
                    continue
                low = low + pltpu.roll(jnp.where(place <= b, got, 0.0), right, 1)
                high = high + pltpu.roll(jnp.where(place > b, got, 0.0), lanes - WIN_LAT * (b + 1), 1)
            for g in range(segs):
                r = (g * WIN_LEVEL + z) * 8
                folds[r:r + WIN_LAT, :SIDE] = low[:, g * SIDE:(g + 1) * SIDE]
                folds[r:r + WIN_LAT, 128:128 + SIDE] = high[:, g * SIDE:(g + 1) * SIDE]
        spread_out = dot(folds[...].astype(BF16), back, NN)
        count = segs * WIN_LEVEL
        for t in range(spots_f.shape[0]):
            spots_f[t] = spread_out[:, t * 128:(t + 1) * 128]
        sums = jnp.zeros((count, spots_f.shape[0] * 128), F32)
        for a in range(WIN_LAT):
            rows = pl.ds(a, count, stride=8)
            got = jnp.concatenate([spots_f[t, rows, :] for t in range(spots_f.shape[0])], axis=1)
            sums = sums + (pltpu.roll(got, a * SPAN, 1) if a else got)
        for t in range(rows_f.shape[0]):
            rows_f[t, :count, :] = sums[:, t * 128:(t + 1) * 128]
        quarters = WIN_LEVEL * WIN_LEVEL
        run = WIN_LAT * PART
        found = []
        for q in range(quarters):
            rows = pl.ds(q, heads, stride=quarters)
            found.append(jnp.concatenate([rows_f[t, rows, :] for t in range(rows_f.shape[0])], axis=1)[:, :run])
        found.append(jnp.zeros((heads, 2 * strip_b - quarters * run), F32))
        full = jnp.concatenate(found, axis=1)
        both = [full[:, :strip_b], full[:, strip_b:], jnp.zeros((8 - 2 * heads, strip_b), F32)]
        bias_cur[0, w * 8:(w + 1) * 8, :] = jnp.concatenate(both, axis=0).astype(BF16)
        return post_b(bias_cur.at[0, pl.ds(w * 8, 8)], bias_in.at[0, pl.ds(w * 8, 8)], mates[0])

    lon_steps = len(lon_bits)

    def bias_total(first, last, flights):
        rows, span = slice(first * 8, last * 8), pl.ds(first * 8, (last - first) * 8)
        for k in range(lon_steps):
            for copy in flights:
                copy.wait_recv()
            fresh = bias_cur[k, rows, :].astype(F32) + bias_in[k, rows, :].astype(F32)
            if k + 1 == lon_steps:
                row = lax.broadcasted_iota(jnp.int32, fresh.shape, 0)
                for w in range(first, last):
                    fresh = jnp.where(row == (w - first) * 8 + 2 * heads, type_ref[0, w].astype(F32), fresh)
            bias_cur[k + 1, rows, :] = fresh.astype(BF16)
            if k + 1 < lon_steps:
                flights = [post_b(bias_cur.at[k + 1, span], bias_in.at[k + 1, span], mates[k + 1])]
        all_bias_ref[pl.ds(lat, 1), rows, :] = bias_cur[lon_steps, rows, :][None]
        return span

    gather_order = list(reversed(list(zip(lat_bits, rows_up))))

    def bias_gather(step, span, have, flights):
        for copy in flights:
            copy.wait_recv()
        bit, device = gather_order[step]
        out = []
        for slot in have:
            src = bias_cur.at[lon_steps, span] if slot is lat else all_bias_ref.at[slot, span]
            out.append(post_b(src, all_bias_ref.at[slot, span], device))
        return have + [flip(slot, bit) for slot in have], out

    lines = []
    for w in range(wins):
        if 0 < w == wins - 1:
            sum_pieces(0)
        window(w)
        if w < wins - 1:
            send_pieces(w)
            lines.append(bias_line(w))
        if w == wins - 2:
            first_rows = slice(0, (wins - 1) * TOK)
            for c in range(4):
                w_acc[c] = dot(gp[first_rows, c * 128:c * 128 + inner], (gs if c == 3 else xs)[first_rows, :], TN)

    last_rows = slice((wins - 1) * TOK, wins * TOK)
    grad_w = [
        w_acc[c] + dot(gp[last_rows, c * 128:c * 128 + inner], (gs if c == 3 else xs)[last_rows, :], TN) for c in range(4)
    ]
    rows_w = 4 * inner
    part_w = rows_w // 2
    for c in range(4):
        first = c * inner
        w_core[first // part_w, first % part_w:first % part_w + inner, :] = grad_w[c].astype(BF16)
    count_w = [0]
    w_copies = []

    def post_w(src, dst, device):
        copy = remote(src, dst, w_sem, count_w[0], device)
        count_w[0] += 1
        copy.start()
        w_copies.append(copy)
        return copy

    keep = lax.rem(lat, 2)
    core_mate = rows_up[0]
    swap = post_w(w_core.at[1 - keep], w_core_in, core_mate)

    if wins > 2:
        sum_pieces(1)
    send_pieces(wins - 1)

    swap.wait_recv()
    sub = part_w // 2
    orders = [
        [(b, m) for b, m in zip(lon_bits, mates)] + [(b, m) for b, m in zip(lat_bits[1:], rows_up[1:])],
        [(b, m) for b, m in zip(lat_bits[1:], rows_up[1:])] + [(b, m) for b, m in zip(lon_bits, mates)],
    ]
    steps = len(orders[0])
    flying = [None, None]
    for j in range(2):
        part = slice(j * sub, (j + 1) * sub)
        w_cur[0, j] = (w_core[keep, part, :].astype(F32) + w_core_in[part, :].astype(F32)).astype(BF16)
        flying[j] = post_w(w_cur.at[0, j], w_in.at[0, j], orders[j][0][1])

    def w_step(k):
        for j in range(2):
            flying[j].wait_recv()
            fresh = (w_cur[k, j].astype(F32) + w_in[k, j].astype(F32)).astype(BF16)
            w_cur[k + 1, j] = fresh
            if k + 1 < steps:
                flying[j] = post_w(w_cur.at[k + 1, j], w_in.at[k + 1, j], orders[j][k + 1][1])

    last_line = bias_line(wins - 1)
    early_span = bias_total(0, wins - 1, lines)
    early_have, early_out = bias_gather(0, early_span, [lat], [])

    order = tail_order(wins, steps, len(gather_order))
    late_have, late_out = [lat], []
    late_span = None
    for task, i in order:
        if task == "piece":
            sum_pieces(i)
        elif task == "w":
            w_step(i)
        elif task == "early":
            early_have, early_out = bias_gather(i, early_span, early_have, early_out)
        elif task == "sum":
            late_span = bias_total(wins - 1, wins, [last_line])
        else:
            late_have, late_out = bias_gather(i, late_span, late_have, late_out)
    both_w = [
        post_w(w_cur.at[steps, j], all_w_ref.at[keep, pl.ds(j * sub, sub)], core_mate) for j in range(2)
    ]
    for j in range(2):
        all_w_ref[pl.ds(keep, 1), j * sub:(j + 1) * sub, :] = w_cur[steps, j][None]
    for copy in both_w + early_out + late_out + edge_copies:
        copy.wait_recv()
    for copy in sent + piece_copies + edge_copies + w_copies + bias_copies:
        copy.wait_send()


def block_backward(reach, unique, x, g, aw, ow, table, types, shift):
    rim = reach * WIN_LAT
    lats_in, cols, levels, width = x.shape
    inner = aw.shape[1]
    heads, _, rel_total = table.shape
    lons, lats, groups = (lax.axis_size(name) for name in ("lon", "lat", "head"))
    wins = levels // WIN_LEVEL
    sides = 1 if lons <= 2 else 2
    lanes = up(heads * TOK, 128)
    tiles = lanes // 128
    block = WIN_LEVEL * WIN_LAT * wins
    rows = up(heads * wins, 16)
    long = up(rel_total + 1, 128)
    lon_steps = len(bits_of(lons))
    steps = lon_steps + len(bits_of(lats)) - 1
    packed = up(MAIN, 16)
    strip = up(rel_total, 256) // 2
    quads = heads * WIN_LEVEL * WIN_LEVEL
    vmem = pl.BlockSpec(memory_space=pltpu.VMEM)
    smem = pl.BlockSpec(memory_space=pltpu.SMEM)
    hbm = pl.BlockSpec(memory_space=pltpu.HBM)
    dma = pltpu.SemaphoreType.DMA
    return pl.pallas_call(
        functools.partial(block_kernel, heads, reach),
        out_shape=(
            pltpu.VMEM((wins, TOK, inner), BF16),
            pltpu.VMEM((sides, wins, 2 * rim, inner), BF16),
            pltpu.VMEM((2, 2 * inner, width), BF16),
            pltpu.VMEM((lats, wins * 8, strip), BF16),
        ),
        in_specs=[smem, smem] + [hbm] * 5,
        out_specs=(vmem,) * 4,
        scratch_shapes=[
            pltpu.VMEM(x.shape, BF16),
            pltpu.VMEM(g.shape, BF16),
            pltpu.VMEM(aw.shape, BF16),
            pltpu.VMEM(ow.shape, BF16),
            pltpu.VMEM(table.shape, F32),
            pltpu.VMEM((2, width // 128, rim * levels, 128), F32),
            pltpu.VMEM((2, width // 128, SIDE * levels, 128), F32),
            pltpu.VMEM((sides, wins, 4 * rim, width), BF16),
            pltpu.VMEM((sides, wins, 4 * rim, width), BF16),
            pltpu.VMEM((wins * TOK, width), BF16),
            pltpu.VMEM((wins * TOK, width), BF16),
            pltpu.VMEM((rows, long), F32),
            pltpu.VMEM((heads * WIN_LEVEL * block, 256), F32),
            pltpu.VMEM((tiles, TOK * wins, 128), F32),
            pltpu.VMEM((tiles, TOK * wins, 128), F32),
            pltpu.VMEM((wins * TOK, 4 * 128), BF16),
            pltpu.VMEM((3 * 128, groups * 128), BF16),
            pltpu.VMEM((wins, groups, packed, 128), BF16),
            pltpu.VMEM((wins, groups - 1, packed, 128), BF16),
            pltpu.VMEM((sides, wins, 2 * rim, inner), BF16),
            pltpu.VMEM((2, 2 * inner, width), BF16),
            pltpu.VMEM((2 * inner, width), BF16),
            pltpu.VMEM((steps + 1, 2, inner, width), BF16),
            pltpu.VMEM((steps, 2, inner, width), BF16),
            pltpu.VMEM((lon_steps + 1, wins * 8, strip), BF16),
            pltpu.VMEM((lon_steps, wins * 8, strip), BF16),
            pltpu.VMEM((4, inner, width), F32),
            pltpu.VMEM((quads * 8, 256), F32),
            pltpu.VMEM((up(WIN_LAT * PART, 128) // 128, quads * 8, 128), F32),
            pltpu.VMEM((up(WIN_LAT * PART, 128) // 128, up(quads, 8), 128), F32),
            dma((5,)),
            dma((2, wins * sides)),
            dma((2, wins * (groups - 1))),
            dma((2, wins * sides)),
            dma((2, 2 * steps + 3)),
            dma((2, wins + 2 * (lon_steps - 1) + 2 * (lats - 1))),
        ],
        compiler_params=pltpu.CompilerParams(
            collective_id=unique, has_side_effects=True, vmem_limit_bytes=54 * 1024 * 1024
        ),
        cost_estimate=pl.CostEstimate(flops=10**9, bytes_accessed=10**7, transcendentals=10**6),
    )(shift, types, x, g, aw, ow, table)


def finish_kernel(reach, shift_ref, own_ref, edge_ref, w_ref, bias_ref,
                  feature_out, aw_out, ow_out, table_out,
                  feature, aw, ow, table, wide, edges, sems):
    shift = shift_ref[0]
    early = shift <= HALF
    rows = reach * WIN_LAT
    wins = own_ref.shape[0]
    chunk = own_ref.shape[2]
    levels = wins * WIN_LEVEL
    sides = edge_ref.shape[0]
    heads, types, total = table.shape
    lats, _, strip = bias_ref.shape
    copies = []

    def put(src, dst):
        copy = pltpu.make_async_copy(src, dst, sems.at[len(copies)])
        copy.start()
        copies.append(copy)

    count = lats * wins
    lines = bias_ref[...].reshape(count * 8, strip)
    kinds = lines[:, :128].astype(F32).reshape(count, 8, 128)[:, 2 * heads:2 * heads + 1, :types]
    kind = lax.broadcasted_iota(jnp.int32, (count, 8, types), 2).astype(F32)
    row = lax.broadcasted_iota(jnp.int32, (count, 8, types), 1)
    same = kinds == kind
    for h in range(heads):
        for p in range(2):
            pick = jnp.where(same & (row == p * heads + h), 1.0, 0.0).reshape(count * 8, types).astype(BF16)
            stop = min(total, (p + 1) * strip)
            table[h, :, p * strip:stop] = dot(pick, lines, TN)[:, :stop - p * strip]
        put(table.at[h], table_out.at[h])

    inner = aw.shape[1]
    flat = w_ref[...].reshape(4 * inner, w_ref.shape[2])
    for c in range(3):
        aw[c] = flat[c * inner:(c + 1) * inner].astype(F32)
    ow[...] = flat[3 * inner:].astype(F32)
    put(aw, aw_out)
    put(ow, ow_out)

    for w in range(wins):
        full = own_ref[w].astype(F32)
        if sides == 1:
            rim = edge_ref[0, w].astype(F32)
        else:
            rim = jnp.where(early, edge_ref[0, w].astype(F32), edge_ref[1, w].astype(F32))
        for z in range(WIN_LEVEL):
            level = WIN_LEVEL * w + z
            wide[pl.ds(level, SIDE, stride=levels), :chunk] = full[z * SIDE:(z + 1) * SIDE]
            edges[pl.ds(level, rows, stride=levels), :chunk] = rim[z * rows:(z + 1) * rows]
    run = WIN_LAT * levels
    for c in range(WIN_LON):
        here = lax.rem(c + WIN_LON - shift, WIN_LON)
        there = jnp.where(early, jnp.maximum(reach + c - shift, 0), jnp.maximum(c - shift, 0))
        there = jnp.minimum(there, reach - 1)
        local = jnp.where(early, (c >= shift).astype(F32), (c < shift).astype(F32)) > 0.5
        near = wide[pl.ds(pl.multiple_of(here * run, 8), run), :]
        far = edges[pl.ds(pl.multiple_of(there * run, 8), run), :]
        mixed = jnp.where(local, near, far)
        feature[:, c] = mixed.reshape(WIN_LAT, levels, 128)[:, :, :chunk].astype(BF16)
    put(feature, feature_out)
    for copy in copies:
        copy.wait()


def finish(reach, own, edge, all_w, all_bias, shift, types, heads, rel_total):
    wins, _, chunk = own.shape
    inner = all_w.shape[1] // 2
    levels = wins * WIN_LEVEL
    vmem = pl.BlockSpec(memory_space=pltpu.VMEM)
    outs = (
        ((WIN_LAT, WIN_LON, levels, chunk), BF16),
        ((3, inner, all_w.shape[2]), F32),
        ((inner, all_w.shape[2]), F32),
        ((heads, types, rel_total), F32),
    )
    return pl.pallas_call(
        functools.partial(finish_kernel, reach),
        out_shape=tuple(jax.ShapeDtypeStruct(*out) for out in outs),
        in_specs=[pl.BlockSpec(memory_space=pltpu.SMEM)] + [vmem] * 4,
        out_specs=(pl.BlockSpec(memory_space=pl.ANY),) * 4,
        scratch_shapes=[pltpu.VMEM(*out) for out in outs] + [
            pltpu.VMEM((SIDE * levels, 128), F32),
            pltpu.VMEM((reach * WIN_LAT * levels, 128), F32),
            pltpu.SemaphoreType.DMA((heads + 3,)),
        ],
        compiler_params=pltpu.CompilerParams(vmem_limit_bytes=20 * 1024 * 1024),
    )(shift, own, edge, all_w, all_bias)


REACHES = (HALF,)


def per_device(features, attend_weight, output_weight, bias_table, bias_type, window_shift, grad_out):
    x, g = (v.transpose(1, 2, 0, 3) for v in (features, grad_out))
    aw = attend_weight.transpose(0, 2, 1)
    table = bias_table.transpose(1, 0, 2)
    types, heads, rel_total = bias_table.shape

    def run(i, x, g, aw, ow, table, kinds, shift):
        gathered = block_backward(REACHES[i], i, x, g, aw, ow, table, kinds, shift)
        return finish(REACHES[i], *gathered, shift, types, heads, rel_total)

    feature_grad, attend_grad, output_grad, bias_grad = run(
        0, x, g, aw, output_weight, table, bias_type.T, window_shift
    )
    return (
        feature_grad.transpose(2, 0, 1, 3),
        attend_grad.transpose(0, 2, 1),
        output_grad,
        bias_grad.transpose(1, 0, 2),
    )


def solution(mesh):
    placed = (
        P(None, "lat", "lon", None),
        P(None, None, "head"),
        P("head", None),
        P(None, "head", None),
        P(None, "lat"),
        P(),
        P(None, "lat", "lon", None),
    )
    return jax.shard_map(
        per_device,
        mesh=mesh,
        in_specs=placed,
        out_specs=(
            P(None, "lat", "lon", "head"),
            P(None, None, "head"),
            P("head", None),
            P(None, "head", None),
        ),
        check_vma=False,
    )
```

```python
import functools

import jax
import jax.numpy as jnp
from jax import lax
from jax.experimental import pallas as pl
from jax.experimental.pallas import tpu as pltpu
from jax.sharding import PartitionSpec as P

WIN_LEVEL = 2
WIN_LAT = 6
WIN_LON = 12
HALF = WIN_LON // 2
SPAN = 2 * WIN_LON - 1
SIDE = WIN_LON * WIN_LAT
TOK = WIN_LEVEL * SIDE
EDGE = HALF * WIN_LAT
MAIN = TOK - EDGE
PART = WIN_LAT * SPAN
LOG2E = 1.4426950408889634
F32 = jnp.float32
BF16 = jnp.bfloat16

NN = ((1,), (0,))
NT = ((1,), (1,))
TN = ((0,), (0,))


def dot(a, b, dims):
    return lax.dot_general(a, b, (dims, ((), ())), preferred_element_type=F32)


def up(n, to):
    return -(-n // to) * to


def bits_of(n):
    return [1 << k for k in range(n.bit_length() - 1)]


def flip(i, bit):
    return i + bit - 2 * bit * lax.rem(i // bit, 2)


def permutation():
    row = lax.broadcasted_iota(jnp.int32, (PART, 256), 0)
    out = lax.broadcasted_iota(jnp.int32, (PART, 256), 1)
    a, d = row // SPAN, row % SPAN
    place = jnp.where(d < WIN_LON, d * WIN_LAT + a, 128 + (d - WIN_LON) * WIN_LAT + a)
    return jnp.where(place == out, 1.0, 0.0).astype(BF16)


def back_permutation(lanes):
    row = lax.broadcasted_iota(jnp.int32, (256, lanes), 0)
    out = lax.broadcasted_iota(jnp.int32, (256, lanes), 1)
    at = row % 128
    d = at // WIN_LAT + jnp.where(row >= 128, WIN_LON, 0)
    hit = (at % WIN_LAT * PART + d == out) & (at < SIDE) & (d < SPAN)
    return jnp.where(hit, 1.0, 0.0).astype(BF16)


def lane_lon(lanes):
    return lax.broadcasted_iota(jnp.int32, (1, lanes), 1) % SIDE // WIN_LAT


def tail_order(wins, steps, gathers):
    tasks = [("piece", w) for w in range(1, wins - 1)]
    tasks += [("w", 0), ("sum", 0), ("late", 0)] + [("early", i) for i in range(1, gathers)]
    tasks += [("piece", wins - 1)] + [("w", k) for k in range(1, steps)] + [("late", i) for i in range(1, gathers)]
    return tasks


def block_kernel(heads, reach, shift_hbm, type_hbm, x_hbm, g_hbm, aw_hbm, ow_hbm, table_hbm,
                 own_ref, edge_ref, all_w_ref, all_bias_ref,
                 x_own, g_own, aw, ow, table, halo_f, own_f, halo_out, halo_in, xs, gs,
                 line, parts, bias, gbias, gp, aw_split, piece_out, piece_in, edge_out,
                 w_core, w_core_in, w_cur, w_in, bias_cur, bias_in, w_acc, folds, spots_f, rows_f,
                 shift_ref, type_ref, local, halo_sem, piece_sem, edge_sem, w_sem, bias_sem):
    lons, lats, groups = (lax.axis_size(name) for name in ("lon", "lat", "head"))
    lon, lat, head = (lax.axis_index(name) for name in ("lon", "lat", "head"))
    rim = reach * WIN_LAT
    cols, levels, width = x_own.shape[1:]
    wins = levels // WIN_LEVEL
    inner = aw.shape[1]
    size = inner // heads
    total = heads * TOK
    lanes = up(total, 128)
    tiles = lanes // 128

    loads = [
        pltpu.make_async_copy(src, dst, local.at[i])
        for i, (src, dst) in enumerate(
            (
                (x_hbm, x_own), (g_hbm, g_own), (table_hbm, table), (aw_hbm, aw), (ow_hbm, ow),
                (type_hbm, type_ref), (shift_hbm, shift_ref),
            )
        )
    ]
    for load in loads[-1:] + loads[:-1]:
        load.start()

    east = (lax.rem(lon + 1, lons), lat, head)
    west = (lax.rem(lon + lons - 1, lons), lat, head)
    lon_bits, lat_bits = bits_of(lons), bits_of(lats)
    mates = [(flip(lon, b), lat, head) for b in lon_bits]
    rows_up = [(lon, flip(lat, b), head) for b in lat_bits]
    sides = [east] if lons <= 2 else [east, west]
    peers = [(lon, lat, lax.rem(head + n, groups)) for n in range(1, groups)]
    greet = sides + (mates if lons > 2 else []) + rows_up + peers
    barrier = pltpu.get_barrier_semaphore()
    for device in greet:
        pl.semaphore_signal(barrier, inc=1, device_id=device, device_id_type=pl.DeviceIdType.MESH)

    def remote(src, dst, sems, k, device):
        return pltpu.make_async_remote_copy(
            src_ref=src, dst_ref=dst, send_sem=sems.at[0, k], recv_sem=sems.at[1, k],
            device_id=device, device_id_type=pl.DeviceIdType.MESH,
        )

    strips = width // 128

    def put(dst, i, spot, value):
        value = value.astype(F32)
        for t in range(strips):
            dst[i, t, spot * levels:(spot + 1) * levels, :] = value[:, t * 128:(t + 1) * 128]

    def take(src, i, level, count):
        rows = pl.ds(level, count, stride=levels)
        return jnp.concatenate([src[i, t, rows, :] for t in range(strips)], axis=1)

    loads[6].wait()
    shift = shift_ref[0]
    early = shift <= HALF
    loads[0].wait()
    loads[1].wait()
    sent = []
    for n in range(len(sides)):
        for i, src in enumerate((x_own, g_own)):
            for b in range(reach):
                low = jnp.maximum(shift + b - reach, 0)
                high = jnp.minimum(shift + b, cols - 1)
                if lons <= 2:
                    col = jnp.where(early, low, high)
                else:
                    col = high if n == 0 else low
                for a in range(WIN_LAT):
                    put(halo_f, i, b * WIN_LAT + a, src[a, col])
        for w in range(wins):
            rows = [take(halo_f, i, WIN_LEVEL * w + z, rim) for i in range(2) for z in range(WIN_LEVEL)]
            halo_out[n, w] = jnp.concatenate(rows, axis=0).astype(BF16)
    pl.semaphore_wait(barrier, len(greet))
    for w in range(wins):
        for n, device in enumerate(sides):
            copy = remote(halo_out.at[n, w], halo_in.at[n, w], halo_sem, w * len(sides) + n, device)
            copy.start()
            sent.append(copy)

    for i, src in enumerate((x_own, g_own)):
        for b in range(WIN_LON):
            col = jnp.where(early, jnp.minimum(shift + b, cols - 1), jnp.maximum(shift + b - WIN_LON, 0))
            for a in range(WIN_LAT):
                put(own_f, i, b * WIN_LAT + a, src[a, col])

    loads[2].wait()
    loads[5].wait()
    parts[...] = jnp.zeros_like(parts)
    for h in range(heads):
        for w in range(wins):
            line[h * wins + w:h * wins + w + 1, :table.shape[2]] = table[h, pl.ds(type_ref[0, w], 1), :]
    block = WIN_LEVEL * WIN_LAT * wins
    spots = []
    for k in range(WIN_LEVEL * WIN_LEVEL * WIN_LAT * WIN_LAT):
        zi, zj = k // (WIN_LEVEL * WIN_LAT * WIN_LAT), k // (WIN_LAT * WIN_LAT) % WIN_LEVEL
        ai, aj = k // WIN_LAT % WIN_LAT, k % WIN_LAT
        for h in range(heads):
            seg = h * WIN_LEVEL + zi
            spots.append((k, h, seg * block + (zj * WIN_LAT + aj) * wins, ai * SPAN))
    for k, h, r, c in spots:
        parts[r:r + wins, c:c + SPAN] = line[h * wins:(h + 1) * wins, k * SPAN:(k + 1) * SPAN]
    perm = permutation()
    flat = parts[:, :PART]
    one = flat.astype(BF16)
    rest = flat - one.astype(F32)
    two = rest.astype(BF16)
    three = (rest - two.astype(F32)).astype(BF16)
    spread = (dot(one, perm, NN) + dot(two, perm, NN) + dot(three, perm, NN)) * LOG2E
    segs = heads * WIN_LEVEL
    pad = jnp.zeros((block, lanes - total), F32)

    def gathered(start):
        pieces = [spread[s * block:(s + 1) * block, start:start + SIDE] for s in range(segs)]
        return jnp.concatenate(pieces + [pad], axis=1)

    lower, upper = gathered(0), gathered(128)
    place = lane_lon(lanes)
    half = WIN_LAT * wins
    for b in range(WIN_LON):
        left = (lanes - WIN_LAT * (WIN_LON - 1 - b)) % lanes
        both = jnp.where(
            place <= b, pltpu.roll(lower, left, 1), pltpu.roll(upper, WIN_LAT * (b + 1), 1)
        )
        for z in range(WIN_LEVEL):
            r = (z * WIN_LON + b) * half
            for t in range(tiles):
                bias[t, r:r + half, :] = both[z * half:(z + 1) * half, t * 128:(t + 1) * 128]

    loads[3].wait()
    loads[4].wait()
    gp[...] = jnp.zeros_like(gp)
    aw_split[...] = jnp.zeros_like(aw_split)
    for c in range(3):
        for g in range(groups):
            aw_split[c * 128:c * 128 + inner, g * 128:g * 128 + inner] = aw[c, :, g * inner:(g + 1) * inner]

    key_lon = lax.broadcasted_iota(jnp.int32, (TOK, 1), 0) % SIDE // WIN_LAT
    mine = jnp.where(early, (key_lon + shift < WIN_LON).astype(F32), (key_lon + shift >= WIN_LON).astype(F32)) > 0.5
    diag = (
        lax.broadcasted_iota(jnp.int32, (inner, lanes), 0) // size
        == lax.broadcasted_iota(jnp.int32, (inner, lanes), 1) // TOK
    )
    col_head = lax.broadcasted_iota(jnp.int32, (TOK, inner), 1) // size
    scaling = size ** -0.5

    def expanded(rows):
        rows = rows.astype(BF16).astype(F32)
        filled = jnp.concatenate([rows] * heads + [jnp.zeros((inner, lanes - total), F32)], axis=1)
        return jnp.where(diag, filled, 0.0).astype(BF16)

    def folded(wide_rows):
        out = jnp.zeros((TOK, inner), F32)
        for h in range(heads):
            out = jnp.where(col_head == h, wide_rows[h * TOK:(h + 1) * TOK], out)
        return out

    piece_copies = []

    def window(w):
        span = slice(w * TOK, (w + 1) * TOK)
        for n in range(len(sides)):
            sent[w * len(sides) + n].wait_recv()
        arrived = [halo_in[n, w].astype(F32) for n in range(len(sides))]
        for i, dst in enumerate((xs, gs)):
            kept = [take(own_f, i, WIN_LEVEL * w + z, SIDE) for z in range(WIN_LEVEL)]
            kept = jnp.concatenate(kept, axis=0)
            near = [got[i * 2 * rim:(i + 1) * 2 * rim] for got in arrived]
            first, last = near[0], near[-1]
            filled = []
            for z in range(WIN_LEVEL):
                part, start = slice(z * rim, (z + 1) * rim), z * SIDE
                filled += [first[part], kept[start + rim:start + SIDE - rim], last[part]]
            filled = jnp.concatenate([f for f in filled if f.shape[0]], axis=0)
            dst[span, :] = jnp.where(mine, kept, filled).astype(BF16)
        tokens, grads = xs[span, :], gs[span, :]
        queries = expanded(dot(aw[0], tokens, NT))
        keys = dot(tokens, aw[1], NT).astype(BF16)
        values = dot(tokens, aw[2], NT).astype(BF16)
        gates = expanded(dot(ow[...], grads, NT))
        rows = pl.ds(w, TOK, stride=wins)
        offset = jnp.concatenate([bias[t, rows, :] for t in range(tiles)], axis=1)
        scores = dot(keys, queries, NN) * (scaling * LOG2E) + offset
        top = jnp.max(scores, axis=0, keepdims=True)
        raised = jnp.exp2(scores - top)
        soft = raised * (1.0 / jnp.sum(raised, axis=0, keepdims=True))
        soft_half = soft.astype(BF16)
        both = soft * dot(values, gates, NN)
        slopes = both - soft * jnp.sum(both, axis=0, keepdims=True)
        for t in range(tiles):
            gbias[t, rows, :] = slopes[:, t * 128:(t + 1) * 128]
        slopes_half = slopes.astype(BF16)
        gp[span, 0 * 128:0 * 128 + inner] = (folded(dot(slopes_half, keys, TN)) * scaling).astype(BF16)
        gp[span, 1 * 128:1 * 128 + inner] = (dot(slopes_half, queries, NT) * scaling).astype(BF16)
        gp[span, 2 * 128:2 * 128 + inner] = dot(soft_half, gates, NT).astype(BF16)
        gp[span, 3 * 128:3 * 128 + inner] = folded(dot(soft_half, values, TN)).astype(BF16)

    def send_pieces(w):
        span = slice(w * TOK, (w + 1) * TOK)
        out = dot(gp[span, :3 * 128], aw_split[...], NN)
        for g in range(groups):
            chunk = out[:, g * 128:g * 128 + inner]
            tail = chunk[MAIN:]
            third = 128 - inner
            extra = jnp.concatenate([tail[:, t * third:(t + 1) * third] for t in range(inner // third)], axis=0)
            packed = jnp.concatenate([chunk[:MAIN], extra], axis=1).astype(BF16)
            piece_out[w, g, :MAIN, :] = packed
        for n, device in enumerate(peers):
            copy = remote(
                piece_out.at[w, device[2]], piece_in.at[w, n], piece_sem, w * len(peers) + n, device
            )
            copy.start()
            piece_copies.append(copy)

    edge_copies = []

    def sum_pieces(w):
        for n in range(len(peers)):
            piece_copies[w * len(peers) + n].wait_recv()
        got = piece_out[w, head].astype(F32)
        for n in range(len(peers)):
            got = got + piece_in[w, n].astype(F32)
        third = 128 - inner
        tail = [got[t * EDGE:(t + 1) * EDGE, inner:] for t in range(inner // third)]
        full = jnp.concatenate([got[:MAIN, :inner], jnp.concatenate(tail, axis=1)], axis=0)
        own_ref[w] = full.astype(BF16)
        first = jnp.concatenate([full[:rim], full[SIDE:SIDE + rim]], axis=0)
        last = jnp.concatenate([full[SIDE - rim:SIDE], full[2 * SIDE - rim:]], axis=0)
        if lons <= 2:
            outs = [jnp.where(early, last, first)]
        else:
            outs = [last, first]
        for n, device in enumerate(sides):
            edge_out[n, w] = outs[n].astype(BF16)
            copy = remote(edge_out.at[n, w], edge_ref.at[n, w], edge_sem, w * len(sides) + n, device)
            copy.start()
            edge_copies.append(copy)

    strip_b = bias_cur.shape[2]
    back = back_permutation(rows_f.shape[0] * 128)
    folds[...] = jnp.zeros_like(folds)
    count_b = [0]
    bias_copies = []

    def post_b(src, dst, device):
        copy = remote(src, dst, bias_sem, count_b[0], device)
        count_b[0] += 1
        copy.start()
        bias_copies.append(copy)
        return copy

    def bias_line(w):
        for z in range(WIN_LEVEL):
            low = jnp.zeros((WIN_LAT, lanes), F32)
            high = jnp.zeros((WIN_LAT, lanes), F32)
            for b in range(WIN_LON):
                rows = pl.ds((z * WIN_LON + b) * half + w, WIN_LAT, stride=wins)
                got = jnp.concatenate([gbias[t, rows, :] for t in range(tiles)], axis=1)
                right = WIN_LAT * (WIN_LON - 1 - b)
                if right == 0:
                    low = low + got
                    continue
                low = low + pltpu.roll(jnp.where(place <= b, got, 0.0), right, 1)
                high = high + pltpu.roll(jnp.where(place > b, got, 0.0), lanes - WIN_LAT * (b + 1), 1)
            for g in range(segs):
                r = (g * WIN_LEVEL + z) * 8
                folds[r:r + WIN_LAT, :SIDE] = low[:, g * SIDE:(g + 1) * SIDE]
                folds[r:r + WIN_LAT, 128:128 + SIDE] = high[:, g * SIDE:(g + 1) * SIDE]
        spread_out = dot(folds[...].astype(BF16), back, NN)
        count = segs * WIN_LEVEL
        for t in range(spots_f.shape[0]):
            spots_f[t] = spread_out[:, t * 128:(t + 1) * 128]
        sums = jnp.zeros((count, spots_f.shape[0] * 128), F32)
        for a in range(WIN_LAT):
            rows = pl.ds(a, count, stride=8)
            got = jnp.concatenate([spots_f[t, rows, :] for t in range(spots_f.shape[0])], axis=1)
            sums = sums + (pltpu.roll(got, a * SPAN, 1) if a else got)
        for t in range(rows_f.shape[0]):
            rows_f[t, :count, :] = sums[:, t * 128:(t + 1) * 128]
        quarters = WIN_LEVEL * WIN_LEVEL
        run = WIN_LAT * PART
        found = []
        for q in range(quarters):
            rows = pl.ds(q, heads, stride=quarters)
            found.append(jnp.concatenate([rows_f[t, rows, :] for t in range(rows_f.shape[0])], axis=1)[:, :run])
        found.append(jnp.zeros((heads, 2 * strip_b - quarters * run), F32))
        full = jnp.concatenate(found, axis=1)
        both = [full[:, :strip_b], full[:, strip_b:], jnp.zeros((8 - 2 * heads, strip_b), F32)]
        bias_cur[0, w * 8:(w + 1) * 8, :] = jnp.concatenate(both, axis=0).astype(BF16)
        return post_b(bias_cur.at[0, pl.ds(w * 8, 8)], bias_in.at[0, pl.ds(w * 8, 8)], mates[0])

    lon_steps = len(lon_bits)

    def bias_total(first, last, flights):
        rows, span = slice(first * 8, last * 8), pl.ds(first * 8, (last - first) * 8)
        for k in range(lon_steps):
            for copy in flights:
                copy.wait_recv()
            fresh = bias_cur[k, rows, :].astype(F32) + bias_in[k, rows, :].astype(F32)
            if k + 1 == lon_steps:
                row = lax.broadcasted_iota(jnp.int32, fresh.shape, 0)
                for w in range(first, last):
                    fresh = jnp.where(row == (w - first) * 8 + 2 * heads, type_ref[0, w].astype(F32), fresh)
            bias_cur[k + 1, rows, :] = fresh.astype(BF16)
            if k + 1 < lon_steps:
                flights = [post_b(bias_cur.at[k + 1, span], bias_in.at[k + 1, span], mates[k + 1])]
        all_bias_ref[pl.ds(lat, 1), rows, :] = bias_cur[lon_steps, rows, :][None]
        return span

    gather_order = list(reversed(list(zip(lat_bits, rows_up))))

    def bias_gather(step, span, have, flights):
        for copy in flights:
            copy.wait_recv()
        bit, device = gather_order[step]
        out = []
        for slot in have:
            src = bias_cur.at[lon_steps, span] if slot is lat else all_bias_ref.at[slot, span]
            out.append(post_b(src, all_bias_ref.at[slot, span], device))
        return have + [flip(slot, bit) for slot in have], out

    lines = []
    for w in range(wins):
        window(w)
        if w < wins - 1:
            send_pieces(w)
            lines.append(bias_line(w))
        if w == wins - 2:
            first_rows = slice(0, (wins - 1) * TOK)
            for c in range(4):
                w_acc[c] = dot(gp[first_rows, c * 128:c * 128 + inner], (gs if c == 3 else xs)[first_rows, :], TN)

    last_rows = slice((wins - 1) * TOK, wins * TOK)
    grad_w = [
        w_acc[c] + dot(gp[last_rows, c * 128:c * 128 + inner], (gs if c == 3 else xs)[last_rows, :], TN) for c in range(4)
    ]
    rows_w = 4 * inner
    part_w = rows_w // 2
    for c in range(4):
        first = c * inner
        w_core[first // part_w, first % part_w:first % part_w + inner, :] = grad_w[c].astype(BF16)
    count_w = [0]
    w_copies = []

    def post_w(src, dst, device):
        copy = remote(src, dst, w_sem, count_w[0], device)
        count_w[0] += 1
        copy.start()
        w_copies.append(copy)
        return copy

    keep = lax.rem(lat, 2)
    core_mate = rows_up[0]
    swap = post_w(w_core.at[1 - keep], w_core_in, core_mate)

    if wins > 1:
        sum_pieces(0)
    send_pieces(wins - 1)

    swap.wait_recv()
    sub = part_w // 2
    orders = [
        [(b, m) for b, m in zip(lon_bits, mates)] + [(b, m) for b, m in zip(lat_bits[1:], rows_up[1:])],
        [(b, m) for b, m in zip(lat_bits[1:], rows_up[1:])] + [(b, m) for b, m in zip(lon_bits, mates)],
    ]
    steps = len(orders[0])
    flying = [None, None]
    for j in range(2):
        part = slice(j * sub, (j + 1) * sub)
        w_cur[0, j] = (w_core[keep, part, :].astype(F32) + w_core_in[part, :].astype(F32)).astype(BF16)
        flying[j] = post_w(w_cur.at[0, j], w_in.at[0, j], orders[j][0][1])

    def w_step(k):
        for j in range(2):
            flying[j].wait_recv()
            fresh = (w_cur[k, j].astype(F32) + w_in[k, j].astype(F32)).astype(BF16)
            w_cur[k + 1, j] = fresh
            if k + 1 < steps:
                flying[j] = post_w(w_cur.at[k + 1, j], w_in.at[k + 1, j], orders[j][k + 1][1])

    last_line = bias_line(wins - 1)
    early_span = bias_total(0, wins - 1, lines)
    early_have, early_out = bias_gather(0, early_span, [lat], [])

    order = tail_order(wins, steps, len(gather_order))
    late_have, late_out = [lat], []
    late_span = None
    for task, i in order:
        if task == "piece":
            sum_pieces(i)
        elif task == "w":
            w_step(i)
        elif task == "early":
            early_have, early_out = bias_gather(i, early_span, early_have, early_out)
        elif task == "sum":
            late_span = bias_total(wins - 1, wins, [last_line])
        else:
            late_have, late_out = bias_gather(i, late_span, late_have, late_out)
    both_w = [
        post_w(w_cur.at[steps, j], all_w_ref.at[keep, pl.ds(j * sub, sub)], core_mate) for j in range(2)
    ]
    for j in range(2):
        all_w_ref[pl.ds(keep, 1), j * sub:(j + 1) * sub, :] = w_cur[steps, j][None]
    for copy in both_w + early_out + late_out + edge_copies:
        copy.wait_recv()
    for copy in sent + piece_copies + edge_copies + w_copies + bias_copies:
        copy.wait_send()


def block_backward(reach, unique, x, g, aw, ow, table, types, shift):
    rim = reach * WIN_LAT
    lats_in, cols, levels, width = x.shape
    inner = aw.shape[1]
    heads, _, rel_total = table.shape
    lons, lats, groups = (lax.axis_size(name) for name in ("lon", "lat", "head"))
    wins = levels // WIN_LEVEL
    sides = 1 if lons <= 2 else 2
    lanes = up(heads * TOK, 128)
    tiles = lanes // 128
    block = WIN_LEVEL * WIN_LAT * wins
    rows = up(heads * wins, 16)
    long = up(rel_total + 1, 128)
    lon_steps = len(bits_of(lons))
    steps = lon_steps + len(bits_of(lats)) - 1
    packed = up(MAIN, 16)
    strip = up(rel_total, 256) // 2
    quads = heads * WIN_LEVEL * WIN_LEVEL
    vmem = pl.BlockSpec(memory_space=pltpu.VMEM)
    hbm = pl.BlockSpec(memory_space=pltpu.HBM)
    dma = pltpu.SemaphoreType.DMA
    return pl.pallas_call(
        functools.partial(block_kernel, heads, reach),
        out_shape=(
            pltpu.VMEM((wins, TOK, inner), BF16),
            pltpu.VMEM((sides, wins, 2 * rim, inner), BF16),
            pltpu.VMEM((2, 2 * inner, width), BF16),
            pltpu.VMEM((lats, wins * 8, strip), BF16),
        ),
        in_specs=[hbm] * 7,
        out_specs=(vmem,) * 4,
        scratch_shapes=[
            pltpu.VMEM(x.shape, BF16),
            pltpu.VMEM(g.shape, BF16),
            pltpu.VMEM(aw.shape, BF16),
            pltpu.VMEM(ow.shape, BF16),
            pltpu.VMEM(table.shape, F32),
            pltpu.VMEM((2, width // 128, rim * levels, 128), F32),
            pltpu.VMEM((2, width // 128, SIDE * levels, 128), F32),
            pltpu.VMEM((sides, wins, 4 * rim, width), BF16),
            pltpu.VMEM((sides, wins, 4 * rim, width), BF16),
            pltpu.VMEM((wins * TOK, width), BF16),
            pltpu.VMEM((wins * TOK, width), BF16),
            pltpu.VMEM((rows, long), F32),
            pltpu.VMEM((heads * WIN_LEVEL * block, 256), F32),
            pltpu.VMEM((tiles, TOK * wins, 128), F32),
            pltpu.VMEM((tiles, TOK * wins, 128), F32),
            pltpu.VMEM((wins * TOK, 4 * 128), BF16),
            pltpu.VMEM((3 * 128, groups * 128), BF16),
            pltpu.VMEM((wins, groups, packed, 128), BF16),
            pltpu.VMEM((wins, groups - 1, packed, 128), BF16),
            pltpu.VMEM((sides, wins, 2 * rim, inner), BF16),
            pltpu.VMEM((2, 2 * inner, width), BF16),
            pltpu.VMEM((2 * inner, width), BF16),
            pltpu.VMEM((steps + 1, 2, inner, width), BF16),
            pltpu.VMEM((steps, 2, inner, width), BF16),
            pltpu.VMEM((lon_steps + 1, wins * 8, strip), BF16),
            pltpu.VMEM((lon_steps, wins * 8, strip), BF16),
            pltpu.VMEM((4, inner, width), F32),
            pltpu.VMEM((quads * 8, 256), F32),
            pltpu.VMEM((up(WIN_LAT * PART, 128) // 128, quads * 8, 128), F32),
            pltpu.VMEM((up(WIN_LAT * PART, 128) // 128, up(quads, 8), 128), F32),
            pltpu.SMEM(shift.shape, jnp.int32),
            pltpu.SMEM(types.shape, jnp.int32),
            dma((7,)),
            dma((2, wins * sides)),
            dma((2, wins * (groups - 1))),
            dma((2, wins * sides)),
            dma((2, 2 * steps + 3)),
            dma((2, wins + 2 * (lon_steps - 1) + 2 * (lats - 1))),
        ],
        compiler_params=pltpu.CompilerParams(
            collective_id=unique, has_side_effects=True, vmem_limit_bytes=54 * 1024 * 1024
        ),
        cost_estimate=pl.CostEstimate(flops=10**9, bytes_accessed=10**7, transcendentals=10**6),
    )(shift, types, x, g, aw, ow, table)


def finish_kernel(reach, shift_hbm, own_ref, edge_ref, w_ref, bias_ref,
                  feature_out, aw_out, ow_out, table_out,
                  feature, aw, ow, table, wide, edges, shift_ref, shift_sem, sems):
    shift_copy = pltpu.make_async_copy(shift_hbm, shift_ref, shift_sem)
    shift_copy.start()
    rows = reach * WIN_LAT
    wins = own_ref.shape[0]
    chunk = own_ref.shape[2]
    levels = wins * WIN_LEVEL
    sides = edge_ref.shape[0]
    heads, types, total = table.shape
    lats, _, strip = bias_ref.shape
    copies = []

    def put(src, dst):
        copy = pltpu.make_async_copy(src, dst, sems.at[len(copies)])
        copy.start()
        copies.append(copy)

    count = lats * wins
    lines = bias_ref[...].reshape(count * 8, strip)
    kinds = lines[:, :128].astype(F32).reshape(count, 8, 128)[:, 2 * heads:2 * heads + 1, :types]
    kind = lax.broadcasted_iota(jnp.int32, (count, 8, types), 2).astype(F32)
    row = lax.broadcasted_iota(jnp.int32, (count, 8, types), 1)
    same = kinds == kind
    for h in range(heads):
        for p in range(2):
            pick = jnp.where(same & (row == p * heads + h), 1.0, 0.0).reshape(count * 8, types).astype(BF16)
            stop = min(total, (p + 1) * strip)
            table[h, :, p * strip:stop] = dot(pick, lines, TN)[:, :stop - p * strip]
        put(table.at[h], table_out.at[h])

    inner = aw.shape[1]
    flat = w_ref[...].reshape(4 * inner, w_ref.shape[2])
    for c in range(3):
        aw[c] = flat[c * inner:(c + 1) * inner].astype(F32)
    ow[...] = flat[3 * inner:].astype(F32)
    put(aw, aw_out)
    put(ow, ow_out)

    shift_copy.wait()
    shift = shift_ref[0]
    early = shift <= HALF

    for w in range(wins):
        full = own_ref[w].astype(F32)
        if sides == 1:
            rim = edge_ref[0, w].astype(F32)
        else:
            rim = jnp.where(early, edge_ref[0, w].astype(F32), edge_ref[1, w].astype(F32))
        for z in range(WIN_LEVEL):
            level = WIN_LEVEL * w + z
            wide[pl.ds(level, SIDE, stride=levels), :chunk] = full[z * SIDE:(z + 1) * SIDE]
            edges[pl.ds(level, rows, stride=levels), :chunk] = rim[z * rows:(z + 1) * rows]
    run = WIN_LAT * levels
    for c in range(WIN_LON):
        here = lax.rem(c + WIN_LON - shift, WIN_LON)
        there = jnp.where(early, jnp.maximum(reach + c - shift, 0), jnp.maximum(c - shift, 0))
        there = jnp.minimum(there, reach - 1)
        local = jnp.where(early, (c >= shift).astype(F32), (c < shift).astype(F32)) > 0.5
        near = wide[pl.ds(pl.multiple_of(here * run, 8), run), :]
        far = edges[pl.ds(pl.multiple_of(there * run, 8), run), :]
        mixed = jnp.where(local, near, far)
        feature[:, c] = mixed.reshape(WIN_LAT, levels, 128)[:, :, :chunk].astype(BF16)
    put(feature, feature_out)
    for copy in copies:
        copy.wait()


def finish(reach, own, edge, all_w, all_bias, shift, types, heads, rel_total):
    wins, _, chunk = own.shape
    inner = all_w.shape[1] // 2
    levels = wins * WIN_LEVEL
    vmem = pl.BlockSpec(memory_space=pltpu.VMEM)
    outs = (
        ((WIN_LAT, WIN_LON, levels, chunk), BF16),
        ((3, inner, all_w.shape[2]), F32),
        ((inner, all_w.shape[2]), F32),
        ((heads, types, rel_total), F32),
    )
    return pl.pallas_call(
        functools.partial(finish_kernel, reach),
        out_shape=tuple(jax.ShapeDtypeStruct(*out) for out in outs),
        in_specs=[pl.BlockSpec(memory_space=pl.ANY)] + [vmem] * 4,
        out_specs=(pl.BlockSpec(memory_space=pl.ANY),) * 4,
        scratch_shapes=[pltpu.VMEM(*out) for out in outs] + [
            pltpu.VMEM((SIDE * levels, 128), F32),
            pltpu.VMEM((reach * WIN_LAT * levels, 128), F32),
            pltpu.SMEM(shift.shape, jnp.int32),
            pltpu.SemaphoreType.DMA,
            pltpu.SemaphoreType.DMA((heads + 3,)),
        ],
        compiler_params=pltpu.CompilerParams(vmem_limit_bytes=20 * 1024 * 1024),
    )(shift, own, edge, all_w, all_bias)


REACHES = (HALF,)


def per_device(features, attend_weight, output_weight, bias_table, bias_type, window_shift, grad_out):
    x, g = (v.transpose(1, 2, 0, 3) for v in (features, grad_out))
    aw = attend_weight.transpose(0, 2, 1)
    table = bias_table.transpose(1, 0, 2)
    types, heads, rel_total = bias_table.shape

    def run(i, x, g, aw, ow, table, kinds, shift):
        gathered = block_backward(REACHES[i], i, x, g, aw, ow, table, kinds, shift)
        return finish(REACHES[i], *gathered, shift, types, heads, rel_total)

    feature_grad, attend_grad, output_grad, bias_grad = run(
        0, x, g, aw, output_weight, table, bias_type.T, window_shift
    )
    return (
        feature_grad.transpose(2, 0, 1, 3),
        attend_grad.transpose(0, 2, 1),
        output_grad,
        bias_grad.transpose(1, 0, 2),
    )


def solution(mesh):
    placed = (
        P(None, "lat", "lon", None),
        P(None, None, "head"),
        P("head", None),
        P(None, "head", None),
        P(None, "lat"),
        P(),
        P(None, "lat", "lon", None),
    )
    return jax.shard_map(
        per_device,
        mesh=mesh,
        in_specs=placed,
        out_specs=(
            P(None, "lat", "lon", "head"),
            P(None, None, "head"),
            P("head", None),
            P(None, "head", None),
        ),
        check_vma=False,
    )
```

```python
import functools

import jax
import jax.numpy as jnp
from jax import lax
from jax.experimental import pallas as pl
from jax.experimental.pallas import tpu as pltpu
from jax.sharding import PartitionSpec as P

WIN_LEVEL = 2
WIN_LAT = 6
WIN_LON = 12
HALF = WIN_LON // 2
SPAN = 2 * WIN_LON - 1
SIDE = WIN_LON * WIN_LAT
TOK = WIN_LEVEL * SIDE
EDGE = HALF * WIN_LAT
MAIN = TOK - EDGE
PART = WIN_LAT * SPAN
LOG2E = 1.4426950408889634
F32 = jnp.float32
BF16 = jnp.bfloat16

NN = ((1,), (0,))
NT = ((1,), (1,))
TN = ((0,), (0,))


def dot(a, b, dims):
    return lax.dot_general(a, b, (dims, ((), ())), preferred_element_type=F32)


def up(n, to):
    return -(-n // to) * to


def bits_of(n):
    return [1 << k for k in range(n.bit_length() - 1)]


def flip(i, bit):
    return i + bit - 2 * bit * lax.rem(i // bit, 2)


def permutation():
    row = lax.broadcasted_iota(jnp.int32, (PART, 256), 0)
    out = lax.broadcasted_iota(jnp.int32, (PART, 256), 1)
    a, d = row // SPAN, row % SPAN
    place = jnp.where(d < WIN_LON, d * WIN_LAT + a, 128 + (d - WIN_LON) * WIN_LAT + a)
    return jnp.where(place == out, 1.0, 0.0).astype(BF16)


def back_permutation(lanes):
    row = lax.broadcasted_iota(jnp.int32, (256, lanes), 0)
    out = lax.broadcasted_iota(jnp.int32, (256, lanes), 1)
    at = row % 128
    d = at // WIN_LAT + jnp.where(row >= 128, WIN_LON, 0)
    hit = (at % WIN_LAT * PART + d == out) & (at < SIDE) & (d < SPAN)
    return jnp.where(hit, 1.0, 0.0).astype(BF16)


def lane_lon(lanes):
    return lax.broadcasted_iota(jnp.int32, (1, lanes), 1) % SIDE // WIN_LAT


def tail_order(wins, steps, gathers):
    tasks = [("piece", w) for w in range(1, wins - 1)]
    tasks += [("w", 0), ("sum", 0), ("late", 0)] + [("early", i) for i in range(1, gathers)]
    tasks += [("piece", wins - 1)] + [("w", k) for k in range(1, steps)] + [("late", i) for i in range(1, gathers)]
    return tasks


def block_kernel(heads, reach, shift_hbm, type_hbm, x_hbm, g_hbm, aw_hbm, ow_hbm, table_hbm,
                 own_ref, edge_ref, all_w_ref, all_bias_ref,
                 x_own, g_own, aw, ow, table, halo_f, own_f, halo_out, halo_in, xs, gs,
                 line, parts, bias, gbias, gp, aw_split, piece_out, piece_in, edge_out,
                 w_core, w_core_in, w_cur, w_in, bias_cur, bias_in, w_acc, folds, spots_f, rows_f,
                 shift_ref, type_ref, local, halo_sem, piece_sem, edge_sem, w_sem, bias_sem):
    lons, lats, groups = (lax.axis_size(name) for name in ("lon", "lat", "head"))
    lon, lat, head = (lax.axis_index(name) for name in ("lon", "lat", "head"))
    rim = reach * WIN_LAT
    cols, levels, width = x_own.shape[1:]
    wins = levels // WIN_LEVEL
    inner = aw.shape[1]
    size = inner // heads
    total = heads * TOK
    lanes = up(total, 128)
    tiles = lanes // 128

    loads = [
        pltpu.make_async_copy(src, dst, local.at[i])
        for i, (src, dst) in enumerate(
            (
                (x_hbm, x_own), (g_hbm, g_own), (table_hbm, table), (aw_hbm, aw), (ow_hbm, ow),
                (type_hbm, type_ref), (shift_hbm, shift_ref),
            )
        )
    ]
    for load in loads[-1:] + loads[:-1]:
        load.start()

    east = (lax.rem(lon + 1, lons), lat, head)
    west = (lax.rem(lon + lons - 1, lons), lat, head)
    lon_bits, lat_bits = bits_of(lons), bits_of(lats)
    mates = [(flip(lon, b), lat, head) for b in lon_bits]
    rows_up = [(lon, flip(lat, b), head) for b in lat_bits]
    sides = [east] if lons <= 2 else [east, west]
    peers = [(lon, lat, lax.rem(head + n, groups)) for n in range(1, groups)]
    greet = sides + (mates if lons > 2 else []) + rows_up + peers
    barrier = pltpu.get_barrier_semaphore()
    for device in greet:
        pl.semaphore_signal(barrier, inc=1, device_id=device, device_id_type=pl.DeviceIdType.MESH)

    def remote(src, dst, sems, k, device):
        return pltpu.make_async_remote_copy(
            src_ref=src, dst_ref=dst, send_sem=sems.at[0, k], recv_sem=sems.at[1, k],
            device_id=device, device_id_type=pl.DeviceIdType.MESH,
        )

    strips = width // 128

    def put(dst, i, spot, value):
        value = value.astype(F32)
        for t in range(strips):
            dst[i, t, spot * levels:(spot + 1) * levels, :] = value[:, t * 128:(t + 1) * 128]

    def take(src, i, level, count):
        rows = pl.ds(level, count, stride=levels)
        return jnp.concatenate([src[i, t, rows, :] for t in range(strips)], axis=1)

    loads[6].wait()
    shift = shift_ref[0]
    early = shift <= HALF
    sent = []
    for n in range(len(sides)):
        for i, src in enumerate((x_own, g_own)):
            if n == 0:
                loads[i].wait()
            for b in range(reach):
                low = jnp.maximum(shift + b - reach, 0)
                high = jnp.minimum(shift + b, cols - 1)
                if lons <= 2:
                    col = jnp.where(early, low, high)
                else:
                    col = high if n == 0 else low
                for a in range(WIN_LAT):
                    put(halo_f, i, b * WIN_LAT + a, src[a, col])
        for w in range(wins):
            rows = [take(halo_f, i, WIN_LEVEL * w + z, rim) for i in range(2) for z in range(WIN_LEVEL)]
            halo_out[n, w] = jnp.concatenate(rows, axis=0).astype(BF16)
    pl.semaphore_wait(barrier, len(greet))
    for w in range(wins):
        for n, device in enumerate(sides):
            copy = remote(halo_out.at[n, w], halo_in.at[n, w], halo_sem, w * len(sides) + n, device)
            copy.start()
            sent.append(copy)

    for i, src in enumerate((x_own, g_own)):
        for b in range(WIN_LON):
            col = jnp.where(early, jnp.minimum(shift + b, cols - 1), jnp.maximum(shift + b - WIN_LON, 0))
            for a in range(WIN_LAT):
                put(own_f, i, b * WIN_LAT + a, src[a, col])

    loads[2].wait()
    loads[5].wait()
    parts[...] = jnp.zeros_like(parts)
    for h in range(heads):
        for w in range(wins):
            line[h * wins + w:h * wins + w + 1, :table.shape[2]] = table[h, pl.ds(type_ref[0, w], 1), :]
    block = WIN_LEVEL * WIN_LAT * wins
    spots = []
    for k in range(WIN_LEVEL * WIN_LEVEL * WIN_LAT * WIN_LAT):
        zi, zj = k // (WIN_LEVEL * WIN_LAT * WIN_LAT), k // (WIN_LAT * WIN_LAT) % WIN_LEVEL
        ai, aj = k // WIN_LAT % WIN_LAT, k % WIN_LAT
        for h in range(heads):
            seg = h * WIN_LEVEL + zi
            spots.append((k, h, seg * block + (zj * WIN_LAT + aj) * wins, ai * SPAN))
    for k, h, r, c in spots:
        parts[r:r + wins, c:c + SPAN] = line[h * wins:(h + 1) * wins, k * SPAN:(k + 1) * SPAN]
    perm = permutation()
    flat = parts[:, :PART]
    one = flat.astype(BF16)
    rest = flat - one.astype(F32)
    two = rest.astype(BF16)
    three = (rest - two.astype(F32)).astype(BF16)
    spread = (dot(one, perm, NN) + dot(two, perm, NN) + dot(three, perm, NN)) * LOG2E
    segs = heads * WIN_LEVEL
    pad = jnp.zeros((block, lanes - total), F32)

    def gathered(start):
        pieces = [spread[s * block:(s + 1) * block, start:start + SIDE] for s in range(segs)]
        return jnp.concatenate(pieces + [pad], axis=1)

    lower, upper = gathered(0), gathered(128)
    place = lane_lon(lanes)
    half = WIN_LAT * wins
    for b in range(WIN_LON):
        left = (lanes - WIN_LAT * (WIN_LON - 1 - b)) % lanes
        both = jnp.where(
            place <= b, pltpu.roll(lower, left, 1), pltpu.roll(upper, WIN_LAT * (b + 1), 1)
        )
        for z in range(WIN_LEVEL):
            r = (z * WIN_LON + b) * half
            for t in range(tiles):
                bias[t, r:r + half, :] = both[z * half:(z + 1) * half, t * 128:(t + 1) * 128]

    loads[3].wait()
    loads[4].wait()
    gp[...] = jnp.zeros_like(gp)
    aw_split[...] = jnp.zeros_like(aw_split)
    for c in range(3):
        for g in range(groups):
            aw_split[c * 128:c * 128 + inner, g * 128:g * 128 + inner] = aw[c, :, g * inner:(g + 1) * inner]

    key_lon = lax.broadcasted_iota(jnp.int32, (TOK, 1), 0) % SIDE // WIN_LAT
    mine = jnp.where(early, (key_lon + shift < WIN_LON).astype(F32), (key_lon + shift >= WIN_LON).astype(F32)) > 0.5
    diag = (
        lax.broadcasted_iota(jnp.int32, (inner, lanes), 0) // size
        == lax.broadcasted_iota(jnp.int32, (inner, lanes), 1) // TOK
    )
    col_head = lax.broadcasted_iota(jnp.int32, (TOK, inner), 1) // size
    scaling = size ** -0.5

    def expanded(rows):
        rows = rows.astype(BF16).astype(F32)
        filled = jnp.concatenate([rows] * heads + [jnp.zeros((inner, lanes - total), F32)], axis=1)
        return jnp.where(diag, filled, 0.0).astype(BF16)

    def folded(wide_rows):
        out = jnp.zeros((TOK, inner), F32)
        for h in range(heads):
            out = jnp.where(col_head == h, wide_rows[h * TOK:(h + 1) * TOK], out)
        return out

    piece_copies = []

    def window(w):
        span = slice(w * TOK, (w + 1) * TOK)
        for n in range(len(sides)):
            sent[w * len(sides) + n].wait_recv()
        arrived = [halo_in[n, w].astype(F32) for n in range(len(sides))]
        for i, dst in enumerate((xs, gs)):
            kept = [take(own_f, i, WIN_LEVEL * w + z, SIDE) for z in range(WIN_LEVEL)]
            kept = jnp.concatenate(kept, axis=0)
            near = [got[i * 2 * rim:(i + 1) * 2 * rim] for got in arrived]
            first, last = near[0], near[-1]
            filled = []
            for z in range(WIN_LEVEL):
                part, start = slice(z * rim, (z + 1) * rim), z * SIDE
                filled += [first[part], kept[start + rim:start + SIDE - rim], last[part]]
            filled = jnp.concatenate([f for f in filled if f.shape[0]], axis=0)
            dst[span, :] = jnp.where(mine, kept, filled).astype(BF16)
        tokens, grads = xs[span, :], gs[span, :]
        queries = expanded(dot(aw[0], tokens, NT))
        keys = dot(tokens, aw[1], NT).astype(BF16)
        values = dot(tokens, aw[2], NT).astype(BF16)
        gates = expanded(dot(ow[...], grads, NT))
        rows = pl.ds(w, TOK, stride=wins)
        offset = jnp.concatenate([bias[t, rows, :] for t in range(tiles)], axis=1)
        scores = dot(keys, queries, NN) * (scaling * LOG2E) + offset
        top = jnp.max(scores, axis=0, keepdims=True)
        raised = jnp.exp2(scores - top)
        soft = raised * (1.0 / jnp.sum(raised, axis=0, keepdims=True))
        soft_half = soft.astype(BF16)
        both = soft * dot(values, gates, NN)
        slopes = both - soft * jnp.sum(both, axis=0, keepdims=True)
        for t in range(tiles):
            gbias[t, rows, :] = slopes[:, t * 128:(t + 1) * 128]
        slopes_half = slopes.astype(BF16)
        gp[span, 0 * 128:0 * 128 + inner] = (folded(dot(slopes_half, keys, TN)) * scaling).astype(BF16)
        gp[span, 1 * 128:1 * 128 + inner] = (dot(slopes_half, queries, NT) * scaling).astype(BF16)
        gp[span, 2 * 128:2 * 128 + inner] = dot(soft_half, gates, NT).astype(BF16)
        gp[span, 3 * 128:3 * 128 + inner] = folded(dot(soft_half, values, TN)).astype(BF16)

    def send_pieces(w):
        span = slice(w * TOK, (w + 1) * TOK)
        out = dot(gp[span, :3 * 128], aw_split[...], NN)
        for g in range(groups):
            chunk = out[:, g * 128:g * 128 + inner]
            tail = chunk[MAIN:]
            third = 128 - inner
            extra = jnp.concatenate([tail[:, t * third:(t + 1) * third] for t in range(inner // third)], axis=0)
            packed = jnp.concatenate([chunk[:MAIN], extra], axis=1).astype(BF16)
            piece_out[w, g, :MAIN, :] = packed
        for n, device in enumerate(peers):
            copy = remote(
                piece_out.at[w, device[2]], piece_in.at[w, n], piece_sem, w * len(peers) + n, device
            )
            copy.start()
            piece_copies.append(copy)

    edge_copies = []

    def sum_pieces(w):
        for n in range(len(peers)):
            piece_copies[w * len(peers) + n].wait_recv()
        got = piece_out[w, head].astype(F32)
        for n in range(len(peers)):
            got = got + piece_in[w, n].astype(F32)
        third = 128 - inner
        tail = [got[t * EDGE:(t + 1) * EDGE, inner:] for t in range(inner // third)]
        full = jnp.concatenate([got[:MAIN, :inner], jnp.concatenate(tail, axis=1)], axis=0)
        own_ref[w] = full.astype(BF16)
        first = jnp.concatenate([full[:rim], full[SIDE:SIDE + rim]], axis=0)
        last = jnp.concatenate([full[SIDE - rim:SIDE], full[2 * SIDE - rim:]], axis=0)
        if lons <= 2:
            outs = [jnp.where(early, last, first)]
        else:
            outs = [last, first]
        for n, device in enumerate(sides):
            edge_out[n, w] = outs[n].astype(BF16)
            copy = remote(edge_out.at[n, w], edge_ref.at[n, w], edge_sem, w * len(sides) + n, device)
            copy.start()
            edge_copies.append(copy)

    strip_b = bias_cur.shape[2]
    back = back_permutation(rows_f.shape[0] * 128)
    folds[...] = jnp.zeros_like(folds)
    count_b = [0]
    bias_copies = []

    def post_b(src, dst, device):
        copy = remote(src, dst, bias_sem, count_b[0], device)
        count_b[0] += 1
        copy.start()
        bias_copies.append(copy)
        return copy

    def bias_line(w):
        for z in range(WIN_LEVEL):
            low = jnp.zeros((WIN_LAT, lanes), F32)
            high = jnp.zeros((WIN_LAT, lanes), F32)
            for b in range(WIN_LON):
                rows = pl.ds((z * WIN_LON + b) * half + w, WIN_LAT, stride=wins)
                got = jnp.concatenate([gbias[t, rows, :] for t in range(tiles)], axis=1)
                right = WIN_LAT * (WIN_LON - 1 - b)
                if right == 0:
                    low = low + got
                    continue
                low = low + pltpu.roll(jnp.where(place <= b, got, 0.0), right, 1)
                high = high + pltpu.roll(jnp.where(place > b, got, 0.0), lanes - WIN_LAT * (b + 1), 1)
            for g in range(segs):
                r = (g * WIN_LEVEL + z) * 8
                folds[r:r + WIN_LAT, :SIDE] = low[:, g * SIDE:(g + 1) * SIDE]
                folds[r:r + WIN_LAT, 128:128 + SIDE] = high[:, g * SIDE:(g + 1) * SIDE]
        spread_out = dot(folds[...].astype(BF16), back, NN)
        count = segs * WIN_LEVEL
        for t in range(spots_f.shape[0]):
            spots_f[t] = spread_out[:, t * 128:(t + 1) * 128]
        sums = jnp.zeros((count, spots_f.shape[0] * 128), F32)
        for a in range(WIN_LAT):
            rows = pl.ds(a, count, stride=8)
            got = jnp.concatenate([spots_f[t, rows, :] for t in range(spots_f.shape[0])], axis=1)
            sums = sums + (pltpu.roll(got, a * SPAN, 1) if a else got)
        for t in range(rows_f.shape[0]):
            rows_f[t, :count, :] = sums[:, t * 128:(t + 1) * 128]
        quarters = WIN_LEVEL * WIN_LEVEL
        run = WIN_LAT * PART
        found = []
        for q in range(quarters):
            rows = pl.ds(q, heads, stride=quarters)
            found.append(jnp.concatenate([rows_f[t, rows, :] for t in range(rows_f.shape[0])], axis=1)[:, :run])
        found.append(jnp.zeros((heads, 2 * strip_b - quarters * run), F32))
        full = jnp.concatenate(found, axis=1)
        both = [full[:, :strip_b], full[:, strip_b:], jnp.zeros((8 - 2 * heads, strip_b), F32)]
        bias_cur[0, w * 8:(w + 1) * 8, :] = jnp.concatenate(both, axis=0).astype(BF16)
        return post_b(bias_cur.at[0, pl.ds(w * 8, 8)], bias_in.at[0, pl.ds(w * 8, 8)], mates[0])

    lon_steps = len(lon_bits)

    def bias_total(first, last, flights):
        rows, span = slice(first * 8, last * 8), pl.ds(first * 8, (last - first) * 8)
        for k in range(lon_steps):
            for copy in flights:
                copy.wait_recv()
            fresh = bias_cur[k, rows, :].astype(F32) + bias_in[k, rows, :].astype(F32)
            if k + 1 == lon_steps:
                row = lax.broadcasted_iota(jnp.int32, fresh.shape, 0)
                for w in range(first, last):
                    fresh = jnp.where(row == (w - first) * 8 + 2 * heads, type_ref[0, w].astype(F32), fresh)
            bias_cur[k + 1, rows, :] = fresh.astype(BF16)
            if k + 1 < lon_steps:
                flights = [post_b(bias_cur.at[k + 1, span], bias_in.at[k + 1, span], mates[k + 1])]
        all_bias_ref[pl.ds(lat, 1), rows, :] = bias_cur[lon_steps, rows, :][None]
        return span

    gather_order = list(reversed(list(zip(lat_bits, rows_up))))

    def bias_gather(step, span, have, flights):
        for copy in flights:
            copy.wait_recv()
        bit, device = gather_order[step]
        out = []
        for slot in have:
            src = bias_cur.at[lon_steps, span] if slot is lat else all_bias_ref.at[slot, span]
            out.append(post_b(src, all_bias_ref.at[slot, span], device))
        return have + [flip(slot, bit) for slot in have], out

    lines = []
    for w in range(wins):
        window(w)
        if w < wins - 1:
            send_pieces(w)
            lines.append(bias_line(w))
        if w == wins - 2:
            first_rows = slice(0, (wins - 1) * TOK)
            for c in range(4):
                w_acc[c] = dot(gp[first_rows, c * 128:c * 128 + inner], (gs if c == 3 else xs)[first_rows, :], TN)

    last_rows = slice((wins - 1) * TOK, wins * TOK)
    grad_w = [
        w_acc[c] + dot(gp[last_rows, c * 128:c * 128 + inner], (gs if c == 3 else xs)[last_rows, :], TN) for c in range(4)
    ]
    rows_w = 4 * inner
    part_w = rows_w // 2
    for c in range(4):
        first = c * inner
        w_core[first // part_w, first % part_w:first % part_w + inner, :] = grad_w[c].astype(BF16)
    count_w = [0]
    w_copies = []

    def post_w(src, dst, device):
        copy = remote(src, dst, w_sem, count_w[0], device)
        count_w[0] += 1
        copy.start()
        w_copies.append(copy)
        return copy

    keep = lax.rem(lat, 2)
    core_mate = rows_up[0]
    swap = post_w(w_core.at[1 - keep], w_core_in, core_mate)

    if wins > 1:
        sum_pieces(0)
    send_pieces(wins - 1)

    swap.wait_recv()
    sub = part_w // 2
    orders = [
        [(b, m) for b, m in zip(lon_bits, mates)] + [(b, m) for b, m in zip(lat_bits[1:], rows_up[1:])],
        [(b, m) for b, m in zip(lat_bits[1:], rows_up[1:])] + [(b, m) for b, m in zip(lon_bits, mates)],
    ]
    steps = len(orders[0])
    flying = [None, None]
    for j in range(2):
        part = slice(j * sub, (j + 1) * sub)
        w_cur[0, j] = (w_core[keep, part, :].astype(F32) + w_core_in[part, :].astype(F32)).astype(BF16)
        flying[j] = post_w(w_cur.at[0, j], w_in.at[0, j], orders[j][0][1])

    def w_step(k):
        for j in range(2):
            flying[j].wait_recv()
            fresh = (w_cur[k, j].astype(F32) + w_in[k, j].astype(F32)).astype(BF16)
            w_cur[k + 1, j] = fresh
            if k + 1 < steps:
                flying[j] = post_w(w_cur.at[k + 1, j], w_in.at[k + 1, j], orders[j][k + 1][1])

    last_line = bias_line(wins - 1)
    early_span = bias_total(0, wins - 1, lines)
    early_have, early_out = bias_gather(0, early_span, [lat], [])

    order = tail_order(wins, steps, len(gather_order))
    late_have, late_out = [lat], []
    late_span = None
    for task, i in order:
        if task == "piece":
            sum_pieces(i)
        elif task == "w":
            w_step(i)
        elif task == "early":
            early_have, early_out = bias_gather(i, early_span, early_have, early_out)
        elif task == "sum":
            late_span = bias_total(wins - 1, wins, [last_line])
        else:
            late_have, late_out = bias_gather(i, late_span, late_have, late_out)
    both_w = [
        post_w(w_cur.at[steps, j], all_w_ref.at[keep, pl.ds(j * sub, sub)], core_mate) for j in range(2)
    ]
    for j in range(2):
        all_w_ref[pl.ds(keep, 1), j * sub:(j + 1) * sub, :] = w_cur[steps, j][None]
    for copy in both_w + early_out + late_out + edge_copies:
        copy.wait_recv()
    for copy in sent + piece_copies + edge_copies + w_copies + bias_copies:
        copy.wait_send()


def block_backward(reach, unique, x, g, aw, ow, table, types, shift):
    rim = reach * WIN_LAT
    lats_in, cols, levels, width = x.shape
    inner = aw.shape[1]
    heads, _, rel_total = table.shape
    lons, lats, groups = (lax.axis_size(name) for name in ("lon", "lat", "head"))
    wins = levels // WIN_LEVEL
    sides = 1 if lons <= 2 else 2
    lanes = up(heads * TOK, 128)
    tiles = lanes // 128
    block = WIN_LEVEL * WIN_LAT * wins
    rows = up(heads * wins, 16)
    long = up(rel_total + 1, 128)
    lon_steps = len(bits_of(lons))
    steps = lon_steps + len(bits_of(lats)) - 1
    packed = up(MAIN, 16)
    strip = up(rel_total, 256) // 2
    quads = heads * WIN_LEVEL * WIN_LEVEL
    vmem = pl.BlockSpec(memory_space=pltpu.VMEM)
    hbm = pl.BlockSpec(memory_space=pltpu.HBM)
    dma = pltpu.SemaphoreType.DMA
    return pl.pallas_call(
        functools.partial(block_kernel, heads, reach),
        out_shape=(
            pltpu.VMEM((wins, TOK, inner), BF16),
            pltpu.VMEM((sides, wins, 2 * rim, inner), BF16),
            pltpu.VMEM((2, 2 * inner, width), BF16),
            pltpu.VMEM((lats, wins * 8, strip), BF16),
        ),
        in_specs=[hbm] * 7,
        out_specs=(vmem,) * 4,
        scratch_shapes=[
            pltpu.VMEM(x.shape, BF16),
            pltpu.VMEM(g.shape, BF16),
            pltpu.VMEM(aw.shape, BF16),
            pltpu.VMEM(ow.shape, BF16),
            pltpu.VMEM(table.shape, F32),
            pltpu.VMEM((2, width // 128, rim * levels, 128), F32),
            pltpu.VMEM((2, width // 128, SIDE * levels, 128), F32),
            pltpu.VMEM((sides, wins, 4 * rim, width), BF16),
            pltpu.VMEM((sides, wins, 4 * rim, width), BF16),
            pltpu.VMEM((wins * TOK, width), BF16),
            pltpu.VMEM((wins * TOK, width), BF16),
            pltpu.VMEM((rows, long), F32),
            pltpu.VMEM((heads * WIN_LEVEL * block, 256), F32),
            pltpu.VMEM((tiles, TOK * wins, 128), F32),
            pltpu.VMEM((tiles, TOK * wins, 128), F32),
            pltpu.VMEM((wins * TOK, 4 * 128), BF16),
            pltpu.VMEM((3 * 128, groups * 128), BF16),
            pltpu.VMEM((wins, groups, packed, 128), BF16),
            pltpu.VMEM((wins, groups - 1, packed, 128), BF16),
            pltpu.VMEM((sides, wins, 2 * rim, inner), BF16),
            pltpu.VMEM((2, 2 * inner, width), BF16),
            pltpu.VMEM((2 * inner, width), BF16),
            pltpu.VMEM((steps + 1, 2, inner, width), BF16),
            pltpu.VMEM((steps, 2, inner, width), BF16),
            pltpu.VMEM((lon_steps + 1, wins * 8, strip), BF16),
            pltpu.VMEM((lon_steps, wins * 8, strip), BF16),
            pltpu.VMEM((4, inner, width), F32),
            pltpu.VMEM((quads * 8, 256), F32),
            pltpu.VMEM((up(WIN_LAT * PART, 128) // 128, quads * 8, 128), F32),
            pltpu.VMEM((up(WIN_LAT * PART, 128) // 128, up(quads, 8), 128), F32),
            pltpu.SMEM(shift.shape, jnp.int32),
            pltpu.SMEM(types.shape, jnp.int32),
            dma((7,)),
            dma((2, wins * sides)),
            dma((2, wins * (groups - 1))),
            dma((2, wins * sides)),
            dma((2, 2 * steps + 3)),
            dma((2, wins + 2 * (lon_steps - 1) + 2 * (lats - 1))),
        ],
        compiler_params=pltpu.CompilerParams(
            collective_id=unique, has_side_effects=True, vmem_limit_bytes=54 * 1024 * 1024
        ),
        cost_estimate=pl.CostEstimate(flops=10**9, bytes_accessed=10**7, transcendentals=10**6),
    )(shift, types, x, g, aw, ow, table)


def finish_kernel(reach, shift_hbm, own_ref, edge_ref, w_ref, bias_ref,
                  feature_out, aw_out, ow_out, table_out,
                  feature, aw, ow, table, wide, edges, shift_ref, shift_sem, sems):
    shift_copy = pltpu.make_async_copy(shift_hbm, shift_ref, shift_sem)
    shift_copy.start()
    rows = reach * WIN_LAT
    wins = own_ref.shape[0]
    chunk = own_ref.shape[2]
    levels = wins * WIN_LEVEL
    sides = edge_ref.shape[0]
    heads, types, total = table.shape
    lats, _, strip = bias_ref.shape
    copies = []

    def put(src, dst):
        copy = pltpu.make_async_copy(src, dst, sems.at[len(copies)])
        copy.start()
        copies.append(copy)

    count = lats * wins
    lines = bias_ref[...].reshape(count * 8, strip)
    kinds = lines[:, :128].astype(F32).reshape(count, 8, 128)[:, 2 * heads:2 * heads + 1, :types]
    kind = lax.broadcasted_iota(jnp.int32, (count, 8, types), 2).astype(F32)
    row = lax.broadcasted_iota(jnp.int32, (count, 8, types), 1)
    same = kinds == kind
    for h in range(heads):
        for p in range(2):
            pick = jnp.where(same & (row == p * heads + h), 1.0, 0.0).reshape(count * 8, types).astype(BF16)
            stop = min(total, (p + 1) * strip)
            table[h, :, p * strip:stop] = dot(pick, lines, TN)[:, :stop - p * strip]
        put(table.at[h], table_out.at[h])

    inner = aw.shape[1]
    flat = w_ref[...].reshape(4 * inner, w_ref.shape[2])
    for c in range(3):
        aw[c] = flat[c * inner:(c + 1) * inner].astype(F32)
    ow[...] = flat[3 * inner:].astype(F32)
    put(aw, aw_out)
    put(ow, ow_out)

    shift_copy.wait()
    shift = shift_ref[0]
    early = shift <= HALF

    for w in range(wins):
        full = own_ref[w].astype(F32)
        if sides == 1:
            rim = edge_ref[0, w].astype(F32)
        else:
            rim = jnp.where(early, edge_ref[0, w].astype(F32), edge_ref[1, w].astype(F32))
        for z in range(WIN_LEVEL):
            level = WIN_LEVEL * w + z
            wide[pl.ds(level, SIDE, stride=levels), :chunk] = full[z * SIDE:(z + 1) * SIDE]
            edges[pl.ds(level, rows, stride=levels), :chunk] = rim[z * rows:(z + 1) * rows]
    run = WIN_LAT * levels
    for c in range(WIN_LON):
        here = lax.rem(c + WIN_LON - shift, WIN_LON)
        there = jnp.where(early, jnp.maximum(reach + c - shift, 0), jnp.maximum(c - shift, 0))
        there = jnp.minimum(there, reach - 1)
        local = jnp.where(early, (c >= shift).astype(F32), (c < shift).astype(F32)) > 0.5
        near = wide[pl.ds(pl.multiple_of(here * run, 8), run), :]
        far = edges[pl.ds(pl.multiple_of(there * run, 8), run), :]
        mixed = jnp.where(local, near, far)
        feature[:, c] = mixed.reshape(WIN_LAT, levels, 128)[:, :, :chunk].astype(BF16)
    put(feature, feature_out)
    for copy in copies:
        copy.wait()


def finish(reach, own, edge, all_w, all_bias, shift, types, heads, rel_total):
    wins, _, chunk = own.shape
    inner = all_w.shape[1] // 2
    levels = wins * WIN_LEVEL
    vmem = pl.BlockSpec(memory_space=pltpu.VMEM)
    outs = (
        ((WIN_LAT, WIN_LON, levels, chunk), BF16),
        ((3, inner, all_w.shape[2]), F32),
        ((inner, all_w.shape[2]), F32),
        ((heads, types, rel_total), F32),
    )
    return pl.pallas_call(
        functools.partial(finish_kernel, reach),
        out_shape=tuple(jax.ShapeDtypeStruct(*out) for out in outs),
        in_specs=[pl.BlockSpec(memory_space=pl.ANY)] + [vmem] * 4,
        out_specs=(pl.BlockSpec(memory_space=pl.ANY),) * 4,
        scratch_shapes=[pltpu.VMEM(*out) for out in outs] + [
            pltpu.VMEM((SIDE * levels, 128), F32),
            pltpu.VMEM((reach * WIN_LAT * levels, 128), F32),
            pltpu.SMEM(shift.shape, jnp.int32),
            pltpu.SemaphoreType.DMA,
            pltpu.SemaphoreType.DMA((heads + 3,)),
        ],
        compiler_params=pltpu.CompilerParams(vmem_limit_bytes=20 * 1024 * 1024),
    )(shift, own, edge, all_w, all_bias)


REACHES = (HALF,)


def per_device(features, attend_weight, output_weight, bias_table, bias_type, window_shift, grad_out):
    x, g = (v.transpose(1, 2, 0, 3) for v in (features, grad_out))
    aw = attend_weight.transpose(0, 2, 1)
    table = bias_table.transpose(1, 0, 2)
    types, heads, rel_total = bias_table.shape

    def run(i, x, g, aw, ow, table, kinds, shift):
        gathered = block_backward(REACHES[i], i, x, g, aw, ow, table, kinds, shift)
        return finish(REACHES[i], *gathered, shift, types, heads, rel_total)

    feature_grad, attend_grad, output_grad, bias_grad = run(
        0, x, g, aw, output_weight, table, bias_type.T, window_shift
    )
    return (
        feature_grad.transpose(2, 0, 1, 3),
        attend_grad.transpose(0, 2, 1),
        output_grad,
        bias_grad.transpose(1, 0, 2),
    )


def solution(mesh):
    placed = (
        P(None, "lat", "lon", None),
        P(None, None, "head"),
        P("head", None),
        P(None, "head", None),
        P(None, "lat"),
        P(),
        P(None, "lat", "lon", None),
    )
    return jax.shard_map(
        per_device,
        mesh=mesh,
        in_specs=placed,
        out_specs=(
            P(None, "lat", "lon", "head"),
            P(None, None, "head"),
            P("head", None),
            P(None, "head", None),
        ),
        check_vma=False,
    )
```
